32 devices in a mesh: batch: 4 (over x, y), group: 8 (over z, core).
Axes of the slice: x: 2, y: 2, z: 4, core: 2. Of those that a mesh axis runs over, the one named last changes fastest.
Arguments:
- sort_keys: float32 [262144], P(('batch', 'group')), parts along dimension 0
- seg_ids: int32 [262144], P(('batch', 'group')), parts along dimension 0
- payload: bfloat16 [262144, 768], P(('batch', 'group')), parts along dimension 0
Outputs:
- output: bfloat16 [262144, 768], P(('batch', 'group')), parts along dimension 0
There are 4 independent parts. The reference program is written for one: setup_inputs(seed, part) draws one part's arguments, and reference() takes and returns one part's arrays. A program takes and returns all parts, laid end to end along the dimension named above; each array names one.
All inputs are finite; a program needn't handle non-finite values.
Results may differ from the reference program's by a relative error of at most 0.00657627.
Values are sent between devices in bfloat16 or wider.
A program may use at most 1 GiB of HBM per device.

```python
import jax
import jax.numpy as jnp
from jax import lax

GROUP = 8
ROWS_DEV = 8192
WIDTH = 768
TOTAL = GROUP * ROWS_DEV
PAIR = ROWS_DEV // GROUP


def combine_runs(left_part, right_part):
    left_flag, left_rows = left_part
    right_flag, right_rows = right_part
    joined = jnp.where(right_flag[..., None], right_rows, left_rows + right_rows)
    return jnp.logical_or(left_flag, right_flag), joined


def draw_layout(base_key):
    phase_key, size_key, tie_key, place_key, cut_key, base_id_key = jax.random.split(base_key, 6)
    half_pair = PAIR // 2
    dev_phase = jax.random.permutation(phase_key, GROUP)
    bound_no = jnp.arange(1, GROUP, dtype=jnp.int32)
    bound_phase = (dev_phase[:, None] + bound_no[None, :]) % GROUP
    shift_size = jax.random.randint(size_key, (GROUP, GROUP - 1), 0, half_pair + 1)
    cut_shift = jnp.where(bound_phase < GROUP // 2, jnp.maximum(shift_size, 1), -shift_size)
    cut_shift = jnp.where(bound_phase == GROUP // 2, 0, cut_shift)
    full_dev = dev_phase == GROUP - 2
    cut_shift = cut_shift.at[:, 0].set(jnp.where(full_dev, -half_pair, cut_shift[:, 0]))
    cut_shift = cut_shift.at[:, 1].set(jnp.where(full_dev, half_pair, cut_shift[:, 1]))
    band_cuts = bound_no[None, :] * PAIR + cut_shift
    local_rank = jnp.arange(ROWS_DEV, dtype=jnp.int32)

    def band_search(cut_row):
        return jnp.searchsorted(cut_row, local_rank, side='right')

    band_of = jax.vmap(band_search)(band_cuts).astype(jnp.int32)
    prev_band = jnp.maximum(band_of - 1, 0)
    band_low = jnp.take_along_axis(band_cuts, prev_band, axis=1)
    band_phase = jnp.take_along_axis(bound_phase, prev_band, axis=1)
    lead_row = (band_of >= 1) & (local_rank[None, :] == band_low) & (band_phase == GROUP // 2)
    tie_break = jax.random.permutation(tie_key, TOTAL).reshape(GROUP, ROWS_DEV)
    rank_score = band_of * (TOTAL + 1) + jnp.where(lead_row, 0, tie_break + 1)
    score_order = jnp.argsort(rank_score.reshape(-1), stable=True)
    global_rank = jnp.argsort(score_order, stable=True).astype(jnp.int32).reshape(GROUP, ROWS_DEV)
    place_keys = jax.random.split(place_key, GROUP)

    def place_rows(row_key):
        return jax.random.permutation(row_key, ROWS_DEV)

    placement = jax.vmap(place_rows)(place_keys)
    rank_at = jnp.take_along_axis(global_rank, placement, axis=1).reshape(TOTAL)
    seg_cuts = jnp.sort(jax.random.randint(cut_key, (GROUP - 1,), 1, TOTAL))
    first_id = jax.random.randint(base_id_key, (), 0, 1000)
    seg_ids = (jnp.searchsorted(seg_cuts, rank_at, side='right') + first_id).astype(jnp.int32)
    return rank_at, seg_ids


def setup_inputs(seed: int = 0, part: int = 0) -> dict:
    base_key = jax.random.fold_in(jax.random.key(seed), part)
    layout_key, payload_key = jax.random.split(base_key, 2)
    rank_at, seg_ids = draw_layout(layout_key)
    centred = (2 * rank_at + 1 - TOTAL).astype(jnp.float32) / TOTAL
    sort_keys = centred * centred * centred
    noise = jax.random.normal(payload_key, (TOTAL, WIDTH), jnp.float32)
    payload = (noise * ROWS_DEV ** -0.5).astype(jnp.bfloat16)
    return {'sort_keys': sort_keys, 'seg_ids': seg_ids, 'payload': payload}


def reference(sort_keys, seg_ids, payload):
    row_pos = jnp.arange(sort_keys.shape[0], dtype=jnp.int32)
    _, seg_sorted, sort_order = lax.sort((sort_keys, seg_ids, row_pos), num_keys=1)
    run_rows = payload[sort_order].astype(jnp.float32)
    first_flag = jnp.ones((1,), dtype=jnp.bool_)
    run_start = jnp.concatenate([first_flag, seg_sorted[1:] != seg_sorted[:-1]])
    _, scanned = lax.associative_scan(combine_runs, (run_start, run_rows))
    _, back_order = lax.sort((sort_order, row_pos), num_keys=1)
    return scanned[back_order].astype(jnp.bfloat16)
```

```python
import functools

import jax
import jax.numpy as jnp
from jax import lax
from jax.experimental import pallas as pl
from jax.experimental.pallas import tpu as pltpu
from jax.sharding import PartitionSpec as P

LANES = 128
BLOCKS = 4
WIDE = LANES // BLOCKS
ROWS_STEP = 32
SUB = 8
SPAN = 128


def lane_block(shape):
    return lax.broadcasted_iota(jnp.int32, shape, 1) // WIDE


def swap_blocks(parts):
    block = lane_block(parts[0].shape)
    odd = (block % 2) == 1
    high = block >= 2
    one = []
    for k in range(0, BLOCKS, 2):
        a, b = parts[k], parts[k + 1]
        one.append(jnp.where(odd, pltpu.roll(b, WIDE, 1), a))
        one.append(jnp.where(odd, b, pltpu.roll(a, LANES - WIDE, 1)))
    out = [None] * BLOCKS
    for k in range(2):
        a, b = one[k], one[k + 2]
        out[k] = jnp.where(high, pltpu.roll(b, 2 * WIDE, 1), a)
        out[k + 2] = jnp.where(high, b, pltpu.roll(a, 2 * WIDE, 1))
    return out


def pack_kernel(src, dst):
    step_rows = src.shape[1]

    def step(k, carry):
        rows = pl.ds(pl.multiple_of(k * ROWS_STEP, ROWS_STEP), ROWS_STEP)
        for t in range(2):
            cols = slice(t * LANES, (t + 1) * LANES)
            parts = [src[q, rows, cols].astype(jnp.float32) for q in range(BLOCKS)]
            for l, part in enumerate(swap_blocks(parts)):
                dst[t * BLOCKS + l, rows, :] = part.astype(jnp.bfloat16)
        return carry

    lax.fori_loop(0, step_rows // ROWS_STEP, step, 0)


def unpack_kernel(src, *refs):
    dst = refs[-1]
    step_rows = src.shape[1]

    def step(k, carry):
        rows = pl.ds(pl.multiple_of(k * ROWS_STEP, ROWS_STEP), ROWS_STEP)
        for t in range(2):
            cols = slice(t * LANES, (t + 1) * LANES)
            parts = [src[t * BLOCKS + l, rows, :].astype(jnp.float32) for l in range(BLOCKS)]
            for q, part in enumerate(swap_blocks(parts)):
                dst[q, rows, cols] = part.astype(jnp.bfloat16)
        return carry

    lax.fori_loop(0, step_rows // ROWS_STEP, step, 0)


def walk_kernel(group_size, order, starts, spans, src, dst, grid_rows):
    packed_rows = src.shape[0]
    quarter = grid_rows.shape[0] // (group_size * BLOCKS)
    per_dev = quarter

    def spread(k, carry):
        base = pl.multiple_of(k * ROWS_STEP, ROWS_STEP)
        dev = base // per_dev
        row = base % per_dev
        data = src[pl.ds(base, ROWS_STEP), :].astype(jnp.float32)
        for q in range(BLOCKS):
            at = pl.multiple_of((dev * BLOCKS + q) * quarter + row, ROWS_STEP)
            moved = data if q == 0 else pltpu.roll(data, LANES - q * WIDE, 1)
            grid_rows[pl.ds(at, ROWS_STEP), :] = moved
        return carry

    lax.fori_loop(0, packed_rows // ROWS_STEP, spread, 0)

    def load(base):
        index = [order[base + u] for u in range(SUB)]
        return index, [grid_rows[pl.ds(i, 1), :] for i in index]

    def plain(n, total):
        base = n * SPAN
        index, rows = load(base)
        for k in range(SPAN // SUB):
            now_index, now_rows = index, rows
            if k + 1 < SPAN // SUB:
                index, rows = load(base + (k + 1) * SUB)
            for g in range(0, SUB, 4):
                a, b, c, d = now_rows[g:g + 4]
                ab = a + b
                abc = ab + c
                abcd = ab + (c + d)
                sums = (total + a, total + ab, total + abc, total + abcd)
                total = sums[3]
                for u in range(4):
                    grid_rows[pl.ds(now_index[g + u], 1), :] = sums[u]
        return total

    def broken(n, total):
        def one(u, total):
            t = n * SPAN + u
            row = pl.ds(order[t], 1)
            new = starts[t // 16]
            fresh = ((new >> (t % 16)) & 1) == 1
            value = grid_rows[row, :]
            total = jnp.where(fresh, value, total + value)
            grid_rows[row, :] = total
            return total

        return lax.fori_loop(0, SPAN, one, total)

    def walk(n, total):
        return lax.cond(spans[0, n] == 0, plain, broken, n, total)

    lax.fori_loop(0, spans.shape[1], walk, jnp.zeros((1, LANES), jnp.float32))

    block = lane_block((ROWS_STEP, LANES))

    def gather(k, carry):
        base = pl.multiple_of(k * ROWS_STEP, ROWS_STEP)
        dev = base // per_dev
        row = base % per_dev
        merged = None
        for q in range(BLOCKS):
            at = pl.multiple_of((dev * BLOCKS + q) * quarter + row, ROWS_STEP)
            data = grid_rows[pl.ds(at, ROWS_STEP), :]
            merged = data if q == 0 else jnp.where(block == q, pltpu.roll(data, q * WIDE, 1), merged)
        dst[pl.ds(base, ROWS_STEP), :] = merged.astype(jnp.bfloat16)
        return carry

    lax.fori_loop(0, packed_rows // ROWS_STEP, gather, 0)


def solution(mesh):
    group_size = mesh.shape['group']

    def per_device(sort_keys, seg_ids, payload):
        rows_dev = sort_keys.shape[0]
        width = payload.shape[1]
        quarter = rows_dev // BLOCKS
        count = group_size * rows_dev
        chunk_cols = group_size * WIDE
        chunks = width // chunk_cols
        tile = min(512, quarter)

        def pack(c, folded):
            return pl.pallas_call(
                pack_kernel, name=f'pack{c}',
                out_shape=jax.ShapeDtypeStruct((group_size, quarter, LANES), jnp.bfloat16),
                grid=(quarter // tile,),
                in_specs=[pl.BlockSpec((BLOCKS, tile, chunk_cols), lambda i: (0, i, c))],
                out_specs=pl.BlockSpec((group_size, tile, LANES), lambda i: (0, i, 0)),
                compiler_params=pltpu.CompilerParams(vmem_limit_bytes=60 * 2**20),
                cost_estimate=pl.CostEstimate(flops=50_000_000, bytes_accessed=2 * rows_dev * chunk_cols * 2,
                                              transcendentals=0),
            )(folded)

        def unpack(c, back, out):
            first = out is None
            return pl.pallas_call(
                unpack_kernel, name=f'unpack{c}',
                out_shape=jax.ShapeDtypeStruct((BLOCKS, quarter, width), jnp.bfloat16),
                grid=(quarter // tile,),
                in_specs=[pl.BlockSpec((group_size, tile, LANES), lambda i: (0, i, 0))]
                + ([] if first else [pl.BlockSpec(memory_space=pl.ANY)]),
                out_specs=pl.BlockSpec((BLOCKS, tile, chunk_cols), lambda i: (0, i, c)),
                input_output_aliases={} if first else {1: 0},
                compiler_params=pltpu.CompilerParams(vmem_limit_bytes=60 * 2**20),
                cost_estimate=pl.CostEstimate(flops=50_000_000, bytes_accessed=2 * rows_dev * chunk_cols * 2,
                                              transcendentals=0),
            )(*((back,) if first else (back, out)))

        def walk(c, order, starts, spans, rows):
            return pl.pallas_call(
                functools.partial(walk_kernel, group_size), name=f'walk{c}',
                out_shape=jax.ShapeDtypeStruct((count // BLOCKS, LANES), jnp.bfloat16),
                in_specs=[pl.BlockSpec(memory_space=pltpu.SMEM)] * 3 + [pl.BlockSpec(memory_space=pltpu.VMEM)],
                out_specs=pl.BlockSpec(memory_space=pltpu.VMEM),
                scratch_shapes=[pltpu.VMEM((count, LANES), jnp.float32)],
                compiler_params=pltpu.CompilerParams(vmem_limit_bytes=60 * 2**20),
                cost_estimate=pl.CostEstimate(flops=1_000_000_000, bytes_accessed=2 * count * WIDE * 2,
                                              transcendentals=0),
            )(order, starts, spans, rows)

        halves = jnp.stack([sort_keys, (seg_ids >> 16).astype(jnp.float32), (seg_ids & 0xFFFF).astype(jnp.float32)])
        every = lax.all_gather(halves, 'group')
        every, folded = lax.optimization_barrier((every, payload.reshape(BLOCKS, quarter, width)))
        keys = every[:, 0].reshape(count)
        ids = ((every[:, 1].astype(jnp.int32) << 16) | every[:, 2].astype(jnp.int32)).reshape(count)
        first = pack(0, folded)
        _, ids_sorted, order = lax.sort((keys, ids, jnp.arange(count, dtype=jnp.int32)), num_keys=1)
        new = jnp.concatenate([jnp.ones((1,), jnp.bool_), ids_sorted[1:] != ids_sorted[:-1]]).astype(jnp.int32)
        starts = jnp.sum(new.reshape(count // 16, 16) << jnp.arange(16, dtype=jnp.int32)[None, :], axis=1)
        spans = jnp.max(new.reshape(1, count // SPAN, SPAN), axis=2)
        order, starts, spans, folded = lax.optimization_barrier((order, starts, spans, folded))

        sent = [first] + [pack(c, folded) for c in range(1, chunks)]
        there = [lax.all_to_all(s, 'group', 0, 0, tiled=True) for s in sent]
        done = [walk(c, order, starts, spans, there[c].reshape(count // BLOCKS, LANES)) for c in range(chunks)]
        back = [lax.all_to_all(d.reshape(group_size, quarter, LANES), 'group', 0, 0, tiled=True) for d in done]
        out = None
        for c in range(chunks):
            out = unpack(c, back[c], out)
        return out.reshape(rows_dev, width)

    row_spec = P(('batch', 'group'))
    mat_spec = P(('batch', 'group'), None)
    return jax.shard_map(per_device, mesh=mesh, in_specs=(row_spec, row_spec, mat_spec),
                         out_specs=mat_spec, check_vma=False)
```

```python
import functools

import jax
import jax.numpy as jnp
from jax import lax
from jax.experimental import pallas as pl
from jax.experimental.pallas import tpu as pltpu
from jax.sharding import PartitionSpec as P

LANES = 128
FOLDS = (2, 4)
PACK_STEP = 128
WALK_STEP = 512
SUB = 8
SPAN = 128


def lane_block(shape, fold):
    return lax.broadcasted_iota(jnp.int32, shape, 1) // (LANES // fold)


def swap_blocks(parts):
    fold = len(parts)
    wide = LANES // fold
    block = lane_block(parts[0].shape, fold)
    reach = 1
    while reach < fold:
        upper = (block // reach) % 2 == 1
        out = [None] * fold
        for k in range(fold):
            if (k // reach) % 2 == 0:
                a, b = parts[k], parts[k + reach]
                out[k] = jnp.where(upper, pltpu.roll(b, reach * wide, 1), a)
                out[k + reach] = jnp.where(upper, b, pltpu.roll(a, LANES - reach * wide, 1))
        parts = out
        reach *= 2
    return parts


def pack_kernel(fold, src, dst):
    step_rows = src.shape[1]

    def step(k, carry):
        rows = pl.ds(pl.multiple_of(k * PACK_STEP, PACK_STEP), PACK_STEP)
        for t in range(dst.shape[0] // fold):
            cols = slice(t * LANES, (t + 1) * LANES)
            parts = [src[q, rows, cols].astype(jnp.float32) for q in range(fold)]
            for l, part in enumerate(swap_blocks(parts)):
                dst[t * fold + l, rows, :] = part.astype(jnp.bfloat16)
        return carry

    lax.fori_loop(0, step_rows // PACK_STEP, step, 0)


def unpack_kernel(fold, src, *refs):
    dst = refs[-1]
    step_rows = src.shape[1]

    def step(k, carry):
        rows = pl.ds(pl.multiple_of(k * PACK_STEP, PACK_STEP), PACK_STEP)
        for t in range(src.shape[0] // fold):
            cols = slice(t * LANES, (t + 1) * LANES)
            parts = [src[t * fold + l, rows, :].astype(jnp.float32) for l in range(fold)]
            for q, part in enumerate(swap_blocks(parts)):
                dst[q, rows, cols] = part.astype(jnp.bfloat16)
        return carry

    lax.fori_loop(0, step_rows // PACK_STEP, step, 0)


def walk_kernel(group_size, fold, order, starts, spans, src, dst, grid_rows):
    packed_rows = src.shape[0]
    part = packed_rows // group_size
    step_rows = min(WALK_STEP, part)
    wide = LANES // fold

    def place(k):
        base = pl.multiple_of(k * step_rows, step_rows)
        dev = base // part
        return base, [pl.multiple_of((dev * fold + q) * part + base % part, step_rows) for q in range(fold)]

    def spread(k, carry):
        base, at = place(k)
        data = src[pl.ds(base, step_rows), :].astype(jnp.float32)
        for q in range(fold):
            grid_rows[pl.ds(at[q], step_rows), :] = data if q == 0 else pltpu.roll(data, LANES - q * wide, 1)
        return carry

    lax.fori_loop(0, packed_rows // step_rows, spread, 0)

    def load(base):
        index = [order[base + u] for u in range(SUB)]
        return index, [grid_rows[pl.ds(i, 1), :] for i in index]

    def plain(n, total):
        base = n * SPAN
        index, rows = load(base)
        for k in range(SPAN // SUB):
            now_index, now_rows = index, rows
            if k + 1 < SPAN // SUB:
                index, rows = load(base + (k + 1) * SUB)
            for g in range(0, SUB, 4):
                a, b, c, d = now_rows[g:g + 4]
                ab = a + b
                abc = ab + c
                abcd = ab + (c + d)
                sums = (total + a, total + ab, total + abc, total + abcd)
                total = sums[3]
                for u in range(4):
                    grid_rows[pl.ds(now_index[g + u], 1), :] = sums[u]
        return total

    def broken(n, total):
        def one(u, total):
            t = n * SPAN + u
            row = pl.ds(order[t], 1)
            new = starts[t // 16]
            fresh = ((new >> (t % 16)) & 1) == 1
            value = grid_rows[row, :]
            total = jnp.where(fresh, value, total + value)
            grid_rows[row, :] = total
            return total

        return lax.fori_loop(0, SPAN, one, total)

    def walk(n, total):
        return lax.cond(spans[0, n] == 0, plain, broken, n, total)

    lax.fori_loop(0, spans.shape[1], walk, jnp.zeros((1, LANES), jnp.float32))

    block = lane_block((step_rows, LANES), fold)

    def merge(k, carry):
        base, at = place(k)
        merged = grid_rows[pl.ds(at[0], step_rows), :]
        for q in range(1, fold):
            moved = pltpu.roll(grid_rows[pl.ds(at[q], step_rows), :], q * wide, 1)
            merged = jnp.where(block == q, moved, merged)
        dst[pl.ds(base, step_rows), :] = merged.astype(jnp.bfloat16)
        return carry

    lax.fori_loop(0, packed_rows // step_rows, merge, 0)


def solution(mesh):
    group_size = mesh.shape['group']

    def per_device(sort_keys, seg_ids, payload):
        rows_dev = sort_keys.shape[0]
        width = payload.shape[1]
        count = group_size * rows_dev
        tile = min(512, rows_dev // max(FOLDS))
        cols = [group_size * (LANES // fold) for fold in FOLDS]
        begin = [sum(cols[:c]) for c in range(len(FOLDS))]

        def estimate(c, flops):
            return pl.CostEstimate(flops=flops, bytes_accessed=4 * rows_dev * cols[c], transcendentals=0)

        def pack(c, rows):
            fold = FOLDS[c]
            part = rows_dev // fold
            return pl.pallas_call(
                functools.partial(pack_kernel, fold), name=f'pack{c}',
                out_shape=jax.ShapeDtypeStruct((group_size, part, LANES), jnp.bfloat16),
                grid=(part // tile,),
                in_specs=[pl.BlockSpec((fold, tile, cols[c]), lambda i: (0, i, begin[c] // cols[c]))],
                out_specs=pl.BlockSpec((group_size, tile, LANES), lambda i: (0, i, 0)),
                compiler_params=pltpu.CompilerParams(vmem_limit_bytes=60 * 2**20),
                cost_estimate=estimate(c, 50_000_000),
            )(rows.reshape(fold, part, width))

        def unpack(c, back, out):
            fold = FOLDS[c]
            part = rows_dev // fold
            first = out is None
            return pl.pallas_call(
                functools.partial(unpack_kernel, fold), name=f'unpack{c}',
                out_shape=jax.ShapeDtypeStruct((fold, part, width), jnp.bfloat16),
                grid=(part // tile,),
                in_specs=[pl.BlockSpec((group_size, tile, LANES), lambda i: (0, i, 0))]
                + ([] if first else [pl.BlockSpec(memory_space=pl.ANY)]),
                out_specs=pl.BlockSpec((fold, tile, cols[c]), lambda i: (0, i, begin[c] // cols[c])),
                input_output_aliases={} if first else {1: 0},
                compiler_params=pltpu.CompilerParams(vmem_limit_bytes=60 * 2**20),
                cost_estimate=estimate(c, 50_000_000),
            )(*((back,) if first else (back, out.reshape(fold, part, width)))).reshape(rows_dev, width)

        def walk(c, order, starts, spans, rows):
            fold = FOLDS[c]
            return pl.pallas_call(
                functools.partial(walk_kernel, group_size, fold), name=f'walk{c}',
                out_shape=jax.ShapeDtypeStruct((count // fold, LANES), jnp.bfloat16),
                in_specs=[pl.BlockSpec(memory_space=pltpu.SMEM)] * 3 + [pl.BlockSpec(memory_space=pltpu.VMEM)],
                out_specs=pl.BlockSpec(memory_space=pltpu.VMEM),
                scratch_shapes=[pltpu.VMEM((count, LANES), jnp.float32)],
                compiler_params=pltpu.CompilerParams(vmem_limit_bytes=62 * 2**20),
                cost_estimate=estimate(c, 1_000_000_000),
            )(order, starts, spans, rows)

        halves = jnp.stack([sort_keys, (seg_ids >> 16).astype(jnp.float32), (seg_ids & 0xFFFF).astype(jnp.float32)])
        every = lax.all_gather(halves, 'group')
        every, folded = lax.optimization_barrier((every, payload))
        keys = every[:, 0].reshape(count)
        ids = ((every[:, 1].astype(jnp.int32) << 16) | every[:, 2].astype(jnp.int32)).reshape(count)
        first = pack(0, folded)
        _, ids_sorted, order = lax.sort((keys, ids, jnp.arange(count, dtype=jnp.int32)), num_keys=1)
        new = jnp.concatenate([jnp.ones((1,), jnp.bool_), ids_sorted[1:] != ids_sorted[:-1]]).astype(jnp.int32)
        starts = jnp.sum(new.reshape(count // 16, 16) << jnp.arange(16, dtype=jnp.int32)[None, :], axis=1)
        spans = jnp.max(new.reshape(1, count // SPAN, SPAN), axis=2)
        order, starts, spans, folded = lax.optimization_barrier((order, starts, spans, folded))

        sent = [first] + [pack(c, folded) for c in range(1, len(FOLDS))]
        there = [lax.all_to_all(s, 'group', 0, 0, tiled=True) for s in sent]
        done = [walk(c, order, starts, spans, t.reshape(-1, LANES)) for c, t in enumerate(there)]
        back = [lax.all_to_all(d.reshape(group_size, -1, LANES), 'group', 0, 0, tiled=True) for d in done]
        out = None
        for c, b in enumerate(back):
            out = unpack(c, b, out)
        return out

    row_spec = P(('batch', 'group'))
    mat_spec = P(('batch', 'group'), None)
    return jax.shard_map(per_device, mesh=mesh, in_specs=(row_spec, row_spec, mat_spec),
                         out_specs=mat_spec, check_vma=False)
```

```python
import functools

import jax
import jax.numpy as jnp
from jax import lax
from jax.experimental import pallas as pl
from jax.experimental.pallas import tpu as pltpu
from jax.sharding import PartitionSpec as P

LANES = 128
FOLDS = (2, 4)
PACK_STEP = 128
WALK_STEP = 512
SUB = 8
SPAN = 128
BITS = 16


def lane_block(shape, fold):
    return lax.broadcasted_iota(jnp.int32, shape, 1) // (LANES // fold)


def swap_blocks(parts):
    fold = len(parts)
    wide = LANES // fold
    block = lane_block(parts[0].shape, fold)
    reach = 1
    while reach < fold:
        upper = (block // reach) % 2 == 1
        out = [None] * fold
        for k in range(fold):
            if (k // reach) % 2 == 0:
                a, b = parts[k], parts[k + reach]
                out[k] = jnp.where(upper, pltpu.roll(b, reach * wide, 1), a)
                out[k + reach] = jnp.where(upper, b, pltpu.roll(a, LANES - reach * wide, 1))
        parts = out
        reach *= 2
    return parts


def pack_kernel(fold, src, dst):
    step_rows = src.shape[1]

    def step(k, carry):
        rows = pl.ds(pl.multiple_of(k * PACK_STEP, PACK_STEP), PACK_STEP)
        for t in range(dst.shape[0] // fold):
            cols = slice(t * LANES, (t + 1) * LANES)
            parts = [src[q, rows, cols].astype(jnp.float32) for q in range(fold)]
            for l, part in enumerate(swap_blocks(parts)):
                dst[t * fold + l, rows, :] = part.astype(jnp.bfloat16)
        return carry

    lax.fori_loop(0, step_rows // PACK_STEP, step, 0)


def unpack_kernel(fold, src, *refs):
    dst = refs[-1]
    step_rows = src.shape[1]

    def step(k, carry):
        rows = pl.ds(pl.multiple_of(k * PACK_STEP, PACK_STEP), PACK_STEP)
        for t in range(src.shape[0] // fold):
            cols = slice(t * LANES, (t + 1) * LANES)
            parts = [src[t * fold + l, rows, :].astype(jnp.float32) for l in range(fold)]
            for q, part in enumerate(swap_blocks(parts)):
                dst[q, rows, cols] = part.astype(jnp.bfloat16)
        return carry

    lax.fori_loop(0, step_rows // PACK_STEP, step, 0)


def walk_kernel(group_size, fold, order_hbm, starts, spans, src, dst, grid_rows, stage, order, in_sem, out_sem, order_sem):
    packed_rows = stage.shape[0]
    part = packed_rows // group_size
    step_rows = min(WALK_STEP, part)
    wide = LANES // fold
    piece = order.shape[0] // group_size
    piece_spans = piece // SPAN

    def part_rows(d):
        return pl.ds(pl.multiple_of(d * part, part), part)

    def copy_in(d):
        return pltpu.make_async_copy(src.at[part_rows(d)], stage.at[part_rows(d)], in_sem.at[d])

    def copy_out(d):
        return pltpu.make_async_copy(stage.at[part_rows(d)], dst.at[part_rows(d)], out_sem.at[d])

    def copy_order(d):
        rows = pl.ds(pl.multiple_of(d * piece, piece), piece)
        return pltpu.make_async_copy(order_hbm.at[rows], order.at[rows], order_sem.at[d])

    for d in range(group_size):
        copy_in(d).start()
    for d in range(group_size):
        copy_order(d).start()

    def place(d, k):
        base = pl.multiple_of(d * part + k * step_rows, step_rows)
        return base, [pl.multiple_of((d * fold + q) * part + k * step_rows, step_rows) for q in range(fold)]

    def spread(d, carry):
        copy_in(d).wait()

        def step(k, carry):
            base, at = place(d, k)
            data = stage[pl.ds(base, step_rows), :].astype(jnp.float32)
            for q in range(fold):
                grid_rows[pl.ds(at[q], step_rows), :] = data if q == 0 else pltpu.roll(data, LANES - q * wide, 1)
            return carry

        return lax.fori_loop(0, part // step_rows, step, carry)

    lax.fori_loop(0, group_size, spread, 0)

    def load(base, rows):
        index = [order[base + u] for u in range(rows)]
        return index, [grid_rows[pl.ds(i, 1), :] for i in index]

    def plain(n, total):
        base = n * SPAN
        index, rows = load(base, SUB)
        for k in range(SPAN // SUB):
            now_index, now_rows = index, rows
            if k + 1 < SPAN // SUB:
                index, rows = load(base + (k + 1) * SUB, SUB)
            for g in range(0, SUB, 4):
                a, b, c, d = now_rows[g:g + 4]
                ab = a + b
                abc = ab + c
                abcd = ab + (c + d)
                sums = (total + a, total + ab, total + abc, total + abcd)
                total = sums[3]
                for u in range(4):
                    grid_rows[pl.ds(now_index[g + u], 1), :] = sums[u]
        return total

    def broken(n, total):
        def sixteen(j, total):
            group = n * (SPAN // BITS) + j
            bits = starts[group]
            index, rows = load(group * BITS, BITS)
            for u in range(BITS):
                total = jnp.where(((bits >> u) & 1) == 1, rows[u], total + rows[u])
                rows[u] = total
            for u in range(BITS):
                grid_rows[pl.ds(index[u], 1), :] = rows[u]
            return total

        return lax.fori_loop(0, SPAN // BITS, sixteen, total)

    def walk(d, total):
        copy_order(d).wait()

        def span(n, total):
            return lax.cond(spans[0, n] == 0, plain, broken, n, total)

        return lax.fori_loop(d * piece_spans, (d + 1) * piece_spans, span, total)

    lax.fori_loop(0, group_size, walk, jnp.zeros((1, LANES), jnp.float32))

    block = lane_block((step_rows, LANES), fold)

    def merge(d, carry):
        def step(k, carry):
            base, at = place(d, k)
            merged = grid_rows[pl.ds(at[0], step_rows), :]
            for q in range(1, fold):
                moved = pltpu.roll(grid_rows[pl.ds(at[q], step_rows), :], q * wide, 1)
                merged = jnp.where(block == q, moved, merged)
            stage[pl.ds(base, step_rows), :] = merged.astype(jnp.bfloat16)
            return carry

        carry = lax.fori_loop(0, part // step_rows, step, carry)
        copy_out(d).start()
        return carry

    lax.fori_loop(0, group_size, merge, 0)
    for d in range(group_size):
        copy_out(d).wait()


def solution(mesh):
    group_size = mesh.shape['group']

    def per_device(sort_keys, seg_ids, payload):
        rows_dev = sort_keys.shape[0]
        width = payload.shape[1]
        count = group_size * rows_dev
        tile = min(512, rows_dev // max(FOLDS))
        cols = [group_size * (LANES // fold) for fold in FOLDS]
        begin = [sum(cols[:c]) for c in range(len(FOLDS))]

        def estimate(c, flops):
            return pl.CostEstimate(flops=flops, bytes_accessed=4 * rows_dev * cols[c], transcendentals=0)

        def pack(c, rows):
            fold = FOLDS[c]
            part = rows_dev // fold
            return pl.pallas_call(
                functools.partial(pack_kernel, fold), name=f'pack{c}',
                out_shape=jax.ShapeDtypeStruct((group_size, part, LANES), jnp.bfloat16),
                grid=(part // tile,),
                in_specs=[pl.BlockSpec((fold, tile, cols[c]), lambda i: (0, i, begin[c] // cols[c]))],
                out_specs=pl.BlockSpec((group_size, tile, LANES), lambda i: (0, i, 0)),
                compiler_params=pltpu.CompilerParams(vmem_limit_bytes=60 * 2**20),
                cost_estimate=estimate(c, 50_000_000),
            )(rows.reshape(fold, part, width))

        def unpack(c, back, out):
            fold = FOLDS[c]
            part = rows_dev // fold
            first = out is None
            return pl.pallas_call(
                functools.partial(unpack_kernel, fold), name=f'unpack{c}',
                out_shape=jax.ShapeDtypeStruct((fold, part, width), jnp.bfloat16),
                grid=(part // tile,),
                in_specs=[pl.BlockSpec((group_size, tile, LANES), lambda i: (0, i, 0))]
                + ([] if first else [pl.BlockSpec(memory_space=pl.ANY)]),
                out_specs=pl.BlockSpec((fold, tile, cols[c]), lambda i: (0, i, begin[c] // cols[c])),
                input_output_aliases={} if first else {1: 0},
                compiler_params=pltpu.CompilerParams(vmem_limit_bytes=60 * 2**20),
                cost_estimate=estimate(c, 50_000_000),
            )(*((back,) if first else (back, out.reshape(fold, part, width)))).reshape(rows_dev, width)

        def walk(c, order, starts, spans, rows):
            fold = FOLDS[c]
            return pl.pallas_call(
                functools.partial(walk_kernel, group_size, fold), name=f'walk{c}',
                out_shape=jax.ShapeDtypeStruct((count // fold, LANES), jnp.bfloat16),
                in_specs=[pl.BlockSpec(memory_space=pl.ANY)] + [pl.BlockSpec(memory_space=pltpu.SMEM)] * 2
                + [pl.BlockSpec(memory_space=pl.ANY)],
                out_specs=pl.BlockSpec(memory_space=pl.ANY),
                scratch_shapes=[
                    pltpu.VMEM((count, LANES), jnp.float32),
                    pltpu.VMEM((count // fold, LANES), jnp.bfloat16),
                    pltpu.SMEM((count,), jnp.int32),
                    pltpu.SemaphoreType.DMA((group_size,)),
                    pltpu.SemaphoreType.DMA((group_size,)),
                    pltpu.SemaphoreType.DMA((group_size,)),
                ],
                compiler_params=pltpu.CompilerParams(vmem_limit_bytes=62 * 2**20),
                cost_estimate=estimate(c, 1_000_000_000),
            )(order, starts, spans, rows)

        halves = jnp.stack([sort_keys, (seg_ids >> 16).astype(jnp.float32), (seg_ids & 0xFFFF).astype(jnp.float32)])
        every = lax.all_gather(halves, 'group')
        every, folded = lax.optimization_barrier((every, payload))
        keys = every[:, 0].reshape(count)
        ids = ((every[:, 1].astype(jnp.int32) << 16) | every[:, 2].astype(jnp.int32)).reshape(count)
        first = pack(0, folded)
        _, ids_sorted, order = lax.sort((keys, ids, jnp.arange(count, dtype=jnp.int32)), num_keys=1)
        new = jnp.concatenate([jnp.ones((1,), jnp.bool_), ids_sorted[1:] != ids_sorted[:-1]]).astype(jnp.int32)
        starts = jnp.sum(new.reshape(count // BITS, BITS) << jnp.arange(BITS, dtype=jnp.int32)[None, :], axis=1)
        spans = jnp.max(new.reshape(1, count // SPAN, SPAN), axis=2)
        order, starts, spans, folded = lax.optimization_barrier((order, starts, spans, folded))

        sent = [first] + [pack(c, folded) for c in range(1, len(FOLDS))]
        there = [lax.all_to_all(s, 'group', 0, 0, tiled=True) for s in sent]
        done = [walk(c, order, starts, spans, t.reshape(-1, LANES)) for c, t in enumerate(there)]
        back = [lax.all_to_all(d.reshape(group_size, -1, LANES), 'group', 0, 0, tiled=True) for d in done]
        out = None
        for c, b in enumerate(back):
            out = unpack(c, b, out)
        return out

    row_spec = P(('batch', 'group'))
    mat_spec = P(('batch', 'group'), None)
    return jax.shard_map(per_device, mesh=mesh, in_specs=(row_spec, row_spec, mat_spec),
                         out_specs=mat_spec, check_vma=False)
```

```python
import functools

import jax
import jax.numpy as jnp
from jax import lax
from jax.experimental import pallas as pl
from jax.experimental.pallas import tpu as pltpu
from jax.sharding import PartitionSpec as P


LANES = 128
FOLDS = (2, 4)
PACK_STEP = 256
WALK_STEP = 1024
SUB = 8
SPAN = 128
BITS = 16


def lane_block(shape, fold):
    return lax.broadcasted_iota(jnp.int32, shape, 1) // (LANES // fold)


def swap_blocks(parts):
    fold = len(parts)
    wide = LANES // fold
    block = lane_block(parts[0].shape, fold)
    reach = 1
    while reach < fold:
        upper = (block // reach) % 2 == 1
        out = [None] * fold
        for k in range(fold):
            if (k // reach) % 2 == 0:
                a, b = parts[k], parts[k + reach]
                out[k] = jnp.where(upper, pltpu.roll(b, reach * wide, 1), a)
                out[k + reach] = jnp.where(upper, b, pltpu.roll(a, LANES - reach * wide, 1))
        parts = out
        reach *= 2
    return parts


def pack_kernel(fold, src, dst):
    step_rows = src.shape[1]

    def step(k, carry):
        rows = pl.ds(pl.multiple_of(k * PACK_STEP, PACK_STEP), PACK_STEP)
        for t in range(dst.shape[0] // fold):
            cols = slice(t * LANES, (t + 1) * LANES)
            parts = [src[q, rows, cols].astype(jnp.float32) for q in range(fold)]
            for l, part in enumerate(swap_blocks(parts)):
                dst[t * fold + l, rows, :] = part.astype(jnp.bfloat16)
        return carry

    lax.fori_loop(0, step_rows // PACK_STEP, step, 0)


def unpack_kernel(fold, src, *refs):
    dst = refs[-1]
    step_rows = src.shape[1]

    def step(k, carry):
        rows = pl.ds(pl.multiple_of(k * PACK_STEP, PACK_STEP), PACK_STEP)
        for t in range(src.shape[0] // fold):
            cols = slice(t * LANES, (t + 1) * LANES)
            parts = [src[t * fold + l, rows, :].astype(jnp.float32) for l in range(fold)]
            for q, part in enumerate(swap_blocks(parts)):
                dst[q, rows, cols] = part.astype(jnp.bfloat16)
        return carry

    lax.fori_loop(0, step_rows // PACK_STEP, step, 0)


def walk_kernel(group_size, fold, order_hbm, starts, spans, src, dst, grid_rows, stage, order, in_sem, out_sem, order_sem):
    packed_rows = stage.shape[0]
    part = packed_rows // group_size
    step_rows = min(WALK_STEP, part)
    wide = LANES // fold
    piece = order.shape[0] // group_size
    piece_spans = piece // SPAN

    def part_rows(d):
        return pl.ds(pl.multiple_of(d * part, part), part)

    def copy_in(d):
        return pltpu.make_async_copy(src.at[part_rows(d)], stage.at[part_rows(d)], in_sem.at[d])

    def copy_out(d):
        return pltpu.make_async_copy(stage.at[part_rows(d)], dst.at[part_rows(d)], out_sem.at[d])

    def copy_order(d):
        rows = pl.ds(pl.multiple_of(d * piece, piece), piece)
        return pltpu.make_async_copy(order_hbm.at[rows], order.at[rows], order_sem.at[d])

    for d in range(group_size):
        copy_in(d).start()
    for d in range(group_size):
        copy_order(d).start()

    def place(d, k):
        base = pl.multiple_of(d * part + k * step_rows, step_rows)
        return base, [pl.multiple_of((d * fold + q) * part + k * step_rows, step_rows) for q in range(fold)]

    def spread(d, carry):
        copy_in(d).wait()

        def step(k, carry):
            base, at = place(d, k)
            data = stage[pl.ds(base, step_rows), :].astype(jnp.float32)
            for q in range(fold):
                grid_rows[pl.ds(at[q], step_rows), :] = data if q == 0 else pltpu.roll(data, LANES - q * wide, 1)
            return carry

        return lax.fori_loop(0, part // step_rows, step, carry)

    lax.fori_loop(0, group_size, spread, 0)

    def load(base, rows):
        index = [order[base + u] for u in range(rows)]
        return index, [grid_rows[pl.ds(i, 1), :] for i in index]

    def sums_of(total, rows):
        out = []
        for g in range(0, len(rows), 4):
            a, b, c, d = rows[g:g + 4]
            ab = a + b
            abc = ab + c
            abcd = ab + (c + d)
            out += [total + a, total + ab, total + abc, total + abcd]
            total = out[-1]
        return out

    def plain(n, total):
        base = n * SPAN
        index, rows = load(base, SUB)
        for k in range(SPAN // SUB):
            now_index, now_rows = index, rows
            if k + 1 < SPAN // SUB:
                index, rows = load(base + (k + 1) * SUB, SUB)
            for i, value in zip(now_index, sums_of(total, now_rows)):
                grid_rows[pl.ds(i, 1), :] = value
                total = value
        return total

    def broken(n, total):
        def whole(group, bits, total):
            index, rows = load(group * BITS, BITS)
            rows = sums_of(total, rows)
            for u in range(BITS):
                grid_rows[pl.ds(index[u], 1), :] = rows[u]
            return rows[-1]

        def cut(group, bits, total):
            index, rows = load(group * BITS, BITS)
            for u in range(BITS):
                total = jnp.where(((bits >> u) & 1) == 1, rows[u], total + rows[u])
                rows[u] = total
            for u in range(BITS):
                grid_rows[pl.ds(index[u], 1), :] = rows[u]
            return total

        def sixteen(j, total):
            group = n * (SPAN // BITS) + j
            bits = starts[group]
            return lax.cond(bits == 0, whole, cut, group, bits, total)

        return lax.fori_loop(0, SPAN // BITS, sixteen, total)

    def walk(d, total):
        copy_order(d).wait()

        def span(n, total):
            return lax.cond(spans[0, n] == 0, plain, broken, n, total)

        return lax.fori_loop(d * piece_spans, (d + 1) * piece_spans, span, total)

    lax.fori_loop(0, group_size, walk, jnp.zeros((1, LANES), jnp.float32))

    block = lane_block((step_rows, LANES), fold)

    def merge(d, carry):
        def step(k, carry):
            base, at = place(d, k)
            merged = grid_rows[pl.ds(at[0], step_rows), :]
            for q in range(1, fold):
                moved = pltpu.roll(grid_rows[pl.ds(at[q], step_rows), :], q * wide, 1)
                merged = jnp.where(block == q, moved, merged)
            stage[pl.ds(base, step_rows), :] = merged.astype(jnp.bfloat16)
            return carry

        carry = lax.fori_loop(0, part // step_rows, step, carry)
        copy_out(d).start()
        return carry

    lax.fori_loop(0, group_size, merge, 0)
    for d in range(group_size):
        copy_out(d).wait()


def solution(mesh):
    group_size = mesh.shape['group']

    def per_device(sort_keys, seg_ids, payload):
        rows_dev = sort_keys.shape[0]
        width = payload.shape[1]
        count = group_size * rows_dev
        tile = min(512, rows_dev // max(FOLDS))
        cols = [group_size * (LANES // fold) for fold in FOLDS]
        begin = [sum(cols[:c]) for c in range(len(FOLDS))]

        def estimate(c, flops):
            return pl.CostEstimate(flops=flops, bytes_accessed=4 * rows_dev * cols[c], transcendentals=0)

        def pack(c, rows):
            fold = FOLDS[c]
            part = rows_dev // fold
            return pl.pallas_call(
                functools.partial(pack_kernel, fold), name=f'pack{c}',
                out_shape=jax.ShapeDtypeStruct((group_size, part, LANES), jnp.bfloat16),
                grid=(part // tile,),
                in_specs=[pl.BlockSpec((fold, tile, cols[c]), lambda i: (0, i, begin[c] // cols[c]))],
                out_specs=pl.BlockSpec((group_size, tile, LANES), lambda i: (0, i, 0)),
                compiler_params=pltpu.CompilerParams(vmem_limit_bytes=60 * 2**20),
                cost_estimate=estimate(c, 50_000_000),
            )(rows.reshape(fold, part, width))

        def unpack(c, back, out):
            fold = FOLDS[c]
            part = rows_dev // fold
            first = out is None
            return pl.pallas_call(
                functools.partial(unpack_kernel, fold), name=f'unpack{c}',
                out_shape=jax.ShapeDtypeStruct((fold, part, width), jnp.bfloat16),
                grid=(part // tile,),
                in_specs=[pl.BlockSpec((group_size, tile, LANES), lambda i: (0, i, 0))]
                + ([] if first else [pl.BlockSpec(memory_space=pl.ANY)]),
                out_specs=pl.BlockSpec((fold, tile, cols[c]), lambda i: (0, i, begin[c] // cols[c])),
                input_output_aliases={} if first else {1: 0},
                compiler_params=pltpu.CompilerParams(vmem_limit_bytes=60 * 2**20),
                cost_estimate=estimate(c, 50_000_000),
            )(*((back,) if first else (back, out.reshape(fold, part, width)))).reshape(rows_dev, width)

        def walk(c, order, starts, spans, rows):
            fold = FOLDS[c]
            return pl.pallas_call(
                functools.partial(walk_kernel, group_size, fold), name=f'walk{c}',
                out_shape=jax.ShapeDtypeStruct((count // fold, LANES), jnp.bfloat16),
                in_specs=[pl.BlockSpec(memory_space=pl.ANY)] + [pl.BlockSpec(memory_space=pltpu.SMEM)] * 2
                + [pl.BlockSpec(memory_space=pl.ANY)],
                out_specs=pl.BlockSpec(memory_space=pl.ANY),
                scratch_shapes=[
                    pltpu.VMEM((count, LANES), jnp.float32),
                    pltpu.VMEM((count // fold, LANES), jnp.bfloat16),
                    pltpu.SMEM((count,), jnp.int32),
                    pltpu.SemaphoreType.DMA((group_size,)),
                    pltpu.SemaphoreType.DMA((group_size,)),
                    pltpu.SemaphoreType.DMA((group_size,)),
                ],
                compiler_params=pltpu.CompilerParams(vmem_limit_bytes=62 * 2**20),
                cost_estimate=estimate(c, 1_000_000_000),
            )(order, starts, spans, rows)

        halves = jnp.stack([sort_keys, (seg_ids >> 16).astype(jnp.float32), (seg_ids & 0xFFFF).astype(jnp.float32)])
        me = lax.axis_index('group')
        shifted = [halves] + [
            lax.ppermute(halves, 'group', [(i, (i + k) % group_size) for i in range(group_size)])
            for k in range(1, group_size)
        ]
        every = jnp.stack(shifted)
        owner = (me - jnp.arange(group_size, dtype=jnp.int32) + group_size) % group_size
        record = (owner[:, None] * rows_dev + jnp.arange(rows_dev, dtype=jnp.int32)[None, :]).reshape(count)
        keys = every[:, 0].reshape(count)
        ids = ((every[:, 1].astype(jnp.int32) << 16) | every[:, 2].astype(jnp.int32)).reshape(count)
        first = pack(0, payload)
        _, ids_sorted, order = lax.sort((keys, ids, record), num_keys=1, is_stable=False)
        new = jnp.concatenate([jnp.ones((1,), jnp.bool_), ids_sorted[1:] != ids_sorted[:-1]]).astype(jnp.int32)
        starts = jnp.sum(new.reshape(count // BITS, BITS) << jnp.arange(BITS, dtype=jnp.int32)[None, :], axis=1)
        spans = jnp.max(new.reshape(1, count // SPAN, SPAN), axis=2)
        order, starts, spans, folded = lax.optimization_barrier((order, starts, spans, payload))

        sent = [first] + [pack(c, folded) for c in range(1, len(FOLDS))]
        there = [lax.all_to_all(s, 'group', 0, 0, tiled=True) for s in sent]
        done = [walk(c, order, starts, spans, t.reshape(-1, LANES)) for c, t in enumerate(there)]
        back = [lax.all_to_all(d.reshape(group_size, -1, LANES), 'group', 0, 0, tiled=True) for d in done]
        out = None
        for c, b in enumerate(back):
            out = unpack(c, b, out)
        return out

    row_spec = P(('batch', 'group'))
    mat_spec = P(('batch', 'group'), None)
    return jax.shard_map(per_device, mesh=mesh, in_specs=(row_spec, row_spec, mat_spec),
                         out_specs=mat_spec, check_vma=False)
```

```python
import functools

import jax
import jax.numpy as jnp
from jax import lax
from jax.experimental import pallas as pl
from jax.experimental.pallas import tpu as pltpu
from jax.sharding import PartitionSpec as P


LANES = 128
FOLDS = (4, 4, 4)
PACK_STEP = 256
WALK_STEP = 1024
SUB = 8
SPAN = 128
BITS = 16


def lane_block(shape, fold):
    return lax.broadcasted_iota(jnp.int32, shape, 1) // (LANES // fold)


def swap_blocks(parts):
    fold = len(parts)
    wide = LANES // fold
    block = lane_block(parts[0].shape, fold)
    reach = 1
    while reach < fold:
        upper = (block // reach) % 2 == 1
        out = [None] * fold
        for k in range(fold):
            if (k // reach) % 2 == 0:
                a, b = parts[k], parts[k + reach]
                out[k] = jnp.where(upper, pltpu.roll(b, reach * wide, 1), a)
                out[k + reach] = jnp.where(upper, b, pltpu.roll(a, LANES - reach * wide, 1))
        parts = out
        reach *= 2
    return parts


def pack_kernel(fold, me, src, *refs):
    *outs, dst = refs
    step_rows = src.shape[1]

    def step(k, carry):
        rows = pl.ds(pl.multiple_of(k * PACK_STEP, PACK_STEP), PACK_STEP)
        for t in range(dst.shape[0] // fold):
            cols = slice(t * LANES, (t + 1) * LANES)
            parts = [src[q, rows, cols].astype(jnp.float32) for q in range(fold)]
            for l, part in enumerate(swap_blocks(parts)):
                dst[t * fold + l, rows, :] = part.astype(jnp.bfloat16)
        return carry

    lax.fori_loop(0, step_rows // PACK_STEP, step, 0)
    for k, out in enumerate(outs):
        out[...] = dst[lax.rem(me[0] + k, len(outs))]


def unpack_kernel(fold, group_size, me, *refs):
    dst, src = refs[-2:]
    for k in range(group_size):
        src[lax.rem(me[0] + k, group_size)] = refs[k][...]
    step_rows = src.shape[1]

    def step(k, carry):
        rows = pl.ds(pl.multiple_of(k * PACK_STEP, PACK_STEP), PACK_STEP)
        for t in range(src.shape[0] // fold):
            cols = slice(t * LANES, (t + 1) * LANES)
            parts = [src[t * fold + l, rows, :].astype(jnp.float32) for l in range(fold)]
            for q, part in enumerate(swap_blocks(parts)):
                dst[q, rows, cols] = part.astype(jnp.bfloat16)
        return carry

    lax.fori_loop(0, step_rows // PACK_STEP, step, 0)


def walk_kernel(group_size, fold, me, order_hbm, starts, spans, *refs):
    srcs, dsts = refs[:group_size], refs[group_size:2 * group_size]
    grid_rows, stage, order, in_sem, out_sem, order_sem = refs[2 * group_size:]
    packed_rows = stage.shape[0]
    part = packed_rows // group_size
    step_rows = min(WALK_STEP, part)
    wide = LANES // fold
    piece = order.shape[0] // group_size
    piece_spans = piece // SPAN

    def part_rows(d):
        return pl.ds(pl.multiple_of(d * part, part), part)

    def owner(k):
        return lax.rem(me[0] - k + group_size, group_size)

    def copy_in(k, src):
        return pltpu.make_async_copy(src, stage.at[part_rows(owner(k))], in_sem.at[k])

    def copy_out(k, dst):
        return pltpu.make_async_copy(stage.at[part_rows(owner(k))], dst, out_sem.at[k])

    def copy_order(d):
        rows = pl.ds(pl.multiple_of(d * piece, piece), piece)
        return pltpu.make_async_copy(order_hbm.at[rows], order.at[rows], order_sem.at[d])

    for k in range(group_size):
        copy_in(k, srcs[k]).start()
    for d in range(group_size):
        copy_order(d).start()

    def place(d, k):
        base = pl.multiple_of(d * part + k * step_rows, step_rows)
        return base, [pl.multiple_of((d * fold + q) * part + k * step_rows, step_rows) for q in range(fold)]

    def spread(j, carry):
        copy_in(j, srcs[0]).wait()
        d = owner(j)

        def step(k, carry):
            base, at = place(d, k)
            data = stage[pl.ds(base, step_rows), :].astype(jnp.float32)
            for q in range(fold):
                grid_rows[pl.ds(at[q], step_rows), :] = data if q == 0 else pltpu.roll(data, LANES - q * wide, 1)
            return carry

        return lax.fori_loop(0, part // step_rows, step, carry)

    lax.fori_loop(0, group_size, spread, 0)

    def load(base, rows):
        index = [order[base + u] for u in range(rows)]
        return index, [grid_rows[pl.ds(i, 1), :] for i in index]

    def sums_of(total, rows):
        out = []
        for g in range(0, len(rows), 4):
            a, b, c, d = rows[g:g + 4]
            ab = a + b
            abc = ab + c
            abcd = ab + (c + d)
            out += [total + a, total + ab, total + abc, total + abcd]
            total = out[-1]
        return out

    def plain(n, total):
        base = n * SPAN
        index, rows = load(base, SUB)
        for k in range(SPAN // SUB):
            now_index, now_rows = index, rows
            if k + 1 < SPAN // SUB:
                index, rows = load(base + (k + 1) * SUB, SUB)
            for i, value in zip(now_index, sums_of(total, now_rows)):
                grid_rows[pl.ds(i, 1), :] = value
                total = value
        return total

    def broken(n, total):
        def whole(group, bits, total):
            index, rows = load(group * BITS, BITS)
            rows = sums_of(total, rows)
            for u in range(BITS):
                grid_rows[pl.ds(index[u], 1), :] = rows[u]
            return rows[-1]

        def cut(group, bits, total):
            index, rows = load(group * BITS, BITS)
            for u in range(BITS):
                total = jnp.where(((bits >> u) & 1) == 1, rows[u], total + rows[u])
                rows[u] = total
            for u in range(BITS):
                grid_rows[pl.ds(index[u], 1), :] = rows[u]
            return total

        def sixteen(j, total):
            group = n * (SPAN // BITS) + j
            bits = starts[group]
            return lax.cond(bits == 0, whole, cut, group, bits, total)

        return lax.fori_loop(0, SPAN // BITS, sixteen, total)

    def walk(d, total):
        copy_order(d).wait()

        def span(n, total):
            return lax.cond(spans[0, n] == 0, plain, broken, n, total)

        return lax.fori_loop(d * piece_spans, (d + 1) * piece_spans, span, total)

    lax.fori_loop(0, group_size, walk, jnp.zeros((1, LANES), jnp.float32))

    block = lane_block((step_rows, LANES), fold)

    def merge(j, carry):
        d = owner(j)

        def step(k, carry):
            base, at = place(d, k)
            merged = grid_rows[pl.ds(at[0], step_rows), :]
            for q in range(1, fold):
                moved = pltpu.roll(grid_rows[pl.ds(at[q], step_rows), :], q * wide, 1)
                merged = jnp.where(block == q, moved, merged)
            stage[pl.ds(base, step_rows), :] = merged.astype(jnp.bfloat16)
            return carry

        carry = lax.fori_loop(0, part // step_rows, step, carry)
        for k in range(group_size):
            @pl.when(j == k)
            def _():
                copy_out(k, dsts[k]).start()
        return carry

    lax.fori_loop(0, group_size, merge, 0)
    for k in range(group_size):
        copy_out(k, dsts[k]).wait()


def solution(mesh):
    group_size = mesh.shape['group']

    def per_device(sort_keys, seg_ids, payload):
        rows_dev = sort_keys.shape[0]
        width = payload.shape[1]
        count = group_size * rows_dev
        tile = min(512, rows_dev // max(FOLDS))
        cols = [group_size * (LANES // fold) for fold in FOLDS]
        begin = [sum(cols[:c]) for c in range(len(FOLDS))]

        def estimate(c, flops):
            return pl.CostEstimate(flops=flops, bytes_accessed=4 * rows_dev * cols[c], transcendentals=0)

        def pack(c, rows):
            fold = FOLDS[c]
            part = rows_dev // fold
            return pl.pallas_call(
                functools.partial(pack_kernel, fold), name=f'pack{c}',
                out_shape=[jax.ShapeDtypeStruct((part, LANES), jnp.bfloat16)] * group_size,
                grid=(part // tile,),
                in_specs=[pl.BlockSpec(memory_space=pltpu.SMEM),
                          pl.BlockSpec((fold, tile, cols[c]), lambda i: (0, i, begin[c] // cols[c]))],
                out_specs=[pl.BlockSpec((tile, LANES), lambda i: (i, 0))] * group_size,
                scratch_shapes=[pltpu.VMEM((group_size, tile, LANES), jnp.bfloat16)],
                compiler_params=pltpu.CompilerParams(vmem_limit_bytes=60 * 2**20),
                cost_estimate=estimate(c, 50_000_000),
            )(place, rows.reshape(fold, part, width))

        def unpack(c, back, out):
            fold = FOLDS[c]
            part = rows_dev // fold
            first = out is None
            return pl.pallas_call(
                functools.partial(unpack_kernel, fold, group_size), name=f'unpack{c}',
                out_shape=jax.ShapeDtypeStruct((fold, part, width), jnp.bfloat16),
                grid=(part // tile,),
                in_specs=[pl.BlockSpec(memory_space=pltpu.SMEM)]
                + [pl.BlockSpec((tile, LANES), lambda i: (i, 0))] * group_size
                + ([] if first else [pl.BlockSpec(memory_space=pl.ANY)]),
                out_specs=pl.BlockSpec((fold, tile, cols[c]), lambda i: (0, i, begin[c] // cols[c])),
                scratch_shapes=[pltpu.VMEM((group_size, tile, LANES), jnp.bfloat16)],
                input_output_aliases={} if first else {1 + group_size: 0},
                compiler_params=pltpu.CompilerParams(vmem_limit_bytes=60 * 2**20),
                cost_estimate=estimate(c, 50_000_000),
            )(place, *back, *(() if first else (out.reshape(fold, part, width),))).reshape(rows_dev, width)

        def walk(c, order, starts, spans, rows):
            fold = FOLDS[c]
            return pl.pallas_call(
                functools.partial(walk_kernel, group_size, fold), name=f'walk{c}',
                out_shape=[jax.ShapeDtypeStruct((rows_dev // fold, LANES), jnp.bfloat16)] * group_size,
                in_specs=[pl.BlockSpec(memory_space=pltpu.SMEM), pl.BlockSpec(memory_space=pl.ANY)]
                + [pl.BlockSpec(memory_space=pltpu.SMEM)] * 2 + [pl.BlockSpec(memory_space=pl.ANY)] * group_size,
                out_specs=[pl.BlockSpec(memory_space=pl.ANY)] * group_size,
                scratch_shapes=[
                    pltpu.VMEM((count, LANES), jnp.float32),
                    pltpu.VMEM((count // fold, LANES), jnp.bfloat16),
                    pltpu.SMEM((count,), jnp.int32),
                    pltpu.SemaphoreType.DMA((group_size,)),
                    pltpu.SemaphoreType.DMA((group_size,)),
                    pltpu.SemaphoreType.DMA((group_size,)),
                ],
                compiler_params=pltpu.CompilerParams(vmem_limit_bytes=62 * 2**20),
                cost_estimate=estimate(c, 1_000_000_000),
            )(place, order, starts, spans, *rows)

        me = lax.axis_index('group')
        place = jnp.full((1,), me, jnp.int32)

        def shift(array, k):
            return lax.ppermute(array, 'group', [(i, (i + k) % group_size) for i in range(group_size)])

        halves = jnp.stack([sort_keys, (seg_ids >> 16).astype(jnp.float32), (seg_ids & 0xFFFF).astype(jnp.float32)])
        shifted = [halves] + [shift(halves, k) for k in range(1, group_size)]
        every = jnp.stack(shifted)
        owner = (me - jnp.arange(group_size, dtype=jnp.int32) + group_size) % group_size
        record = (owner[:, None] * rows_dev + jnp.arange(rows_dev, dtype=jnp.int32)[None, :]).reshape(count)
        keys = every[:, 0].reshape(count)
        ids = ((every[:, 1].astype(jnp.int32) << 16) | every[:, 2].astype(jnp.int32)).reshape(count)
        first = pack(0, payload)
        _, ids_sorted, order = lax.sort((keys, ids, record), num_keys=1, is_stable=False)
        new = jnp.concatenate([jnp.ones((1,), jnp.bool_), ids_sorted[1:] != ids_sorted[:-1]]).astype(jnp.int32)
        starts = jnp.sum(new.reshape(count // BITS, BITS) << jnp.arange(BITS, dtype=jnp.int32)[None, :], axis=1)
        spans = jnp.max(new.reshape(1, count // SPAN, SPAN), axis=2)
        order, starts, spans, folded = lax.optimization_barrier((order, starts, spans, payload))

        sent = [first] + [pack(c, folded) for c in range(1, len(FOLDS))]
        there = [[s[0]] + [shift(s[k], k) for k in range(1, group_size)] for s in sent]
        done = [walk(c, order, starts, spans, t) for c, t in enumerate(there)]
        back = [[d[0]] + [shift(d[k], group_size - k) for k in range(1, group_size)] for d in done]
        out = None
        for c, b in enumerate(back):
            out = unpack(c, b, out)
        return out

    row_spec = P(('batch', 'group'))
    mat_spec = P(('batch', 'group'), None)
    return jax.shard_map(per_device, mesh=mesh, in_specs=(row_spec, row_spec, mat_spec),
                         out_specs=mat_spec, check_vma=False)
```

```python
import functools

import jax
import jax.numpy as jnp
from jax import lax
from jax.experimental import pallas as pl
from jax.experimental.pallas import tpu as pltpu
from jax.sharding import PartitionSpec as P


LANES = 128
FOLDS = (4, 4, 4)
PACK_STEP = 256
WALK_STEP = 1024
BATCHES = (8,) * 16
SPAN = sum(BATCHES)
BITS = 16


def lane_block(shape, fold):
    return lax.broadcasted_iota(jnp.int32, shape, 1) // (LANES // fold)


def swap_blocks(parts):
    fold = len(parts)
    wide = LANES // fold
    block = lane_block(parts[0].shape, fold)
    reach = 1
    while reach < fold:
        upper = (block // reach) % 2 == 1
        out = [None] * fold
        for k in range(fold):
            if (k // reach) % 2 == 0:
                a, b = parts[k], parts[k + reach]
                out[k] = jnp.where(upper, pltpu.roll(b, reach * wide, 1), a)
                out[k + reach] = jnp.where(upper, b, pltpu.roll(a, LANES - reach * wide, 1))
        parts = out
        reach *= 2
    return parts


def pack_kernel(fold, me, src, *refs):
    *outs, dst = refs
    step_rows = src.shape[1]

    def step(k, carry):
        rows = pl.ds(pl.multiple_of(k * PACK_STEP, PACK_STEP), PACK_STEP)
        for t in range(dst.shape[0] // fold):
            cols = slice(t * LANES, (t + 1) * LANES)
            parts = [src[q, rows, cols].astype(jnp.float32) for q in range(fold)]
            for l, part in enumerate(swap_blocks(parts)):
                dst[t * fold + l, rows, :] = part.astype(jnp.bfloat16)
        return carry

    lax.fori_loop(0, step_rows // PACK_STEP, step, 0)
    for k, out in enumerate(outs):
        out[...] = dst[lax.rem(me[0] + k, len(outs))]


def unpack_kernel(fold, group_size, me, *refs):
    dst, src = refs[-2:]
    for k in range(group_size):
        src[lax.rem(me[0] + k, group_size)] = refs[k][...]
    step_rows = src.shape[1]

    def step(k, carry):
        rows = pl.ds(pl.multiple_of(k * PACK_STEP, PACK_STEP), PACK_STEP)
        for t in range(src.shape[0] // fold):
            cols = slice(t * LANES, (t + 1) * LANES)
            parts = [src[t * fold + l, rows, :].astype(jnp.float32) for l in range(fold)]
            for q, part in enumerate(swap_blocks(parts)):
                dst[q, rows, cols] = part.astype(jnp.bfloat16)
        return carry

    lax.fori_loop(0, step_rows // PACK_STEP, step, 0)


def walk_kernel(group_size, fold, me, order_hbm, starts, spans, *refs):
    srcs, dsts = refs[:group_size], refs[group_size:2 * group_size]
    grid_rows, stage, order, in_sem, out_sem, order_sem = refs[2 * group_size:]
    packed_rows = stage.shape[0]
    part = packed_rows // group_size
    step_rows = min(WALK_STEP, part)
    wide = LANES // fold
    piece = order.shape[0] // group_size
    piece_spans = piece // SPAN

    def part_rows(d):
        return pl.ds(pl.multiple_of(d * part, part), part)

    def owner(k):
        return lax.rem(me[0] - k + group_size, group_size)

    def copy_in(k, src):
        return pltpu.make_async_copy(src, stage.at[part_rows(owner(k))], in_sem.at[k])

    def copy_out(k, dst):
        return pltpu.make_async_copy(stage.at[part_rows(owner(k))], dst, out_sem.at[k])

    def copy_order(d):
        rows = pl.ds(pl.multiple_of(d * piece, piece), piece)
        return pltpu.make_async_copy(order_hbm.at[rows], order.at[rows], order_sem.at[d])

    for k in range(group_size):
        copy_in(k, srcs[k]).start()
    for d in range(group_size):
        copy_order(d).start()

    def place(d, k):
        base = pl.multiple_of(d * part + k * step_rows, step_rows)
        return base, [pl.multiple_of((d * fold + q) * part + k * step_rows, step_rows) for q in range(fold)]

    def spread(j, carry):
        copy_in(j, srcs[0]).wait()
        d = owner(j)

        def step(k, carry):
            base, at = place(d, k)
            data = stage[pl.ds(base, step_rows), :].astype(jnp.float32)
            for q in range(fold):
                grid_rows[pl.ds(at[q], step_rows), :] = data if q == 0 else pltpu.roll(data, LANES - q * wide, 1)
            return carry

        return lax.fori_loop(0, part // step_rows, step, carry)

    lax.fori_loop(0, group_size, spread, 0)

    def load(base, rows):
        index = [order[base + u] for u in range(rows)]
        return index, [grid_rows[pl.ds(i, 1), :] for i in index]

    def sums_of(total, rows):
        out = []
        for g in range(0, len(rows), 4):
            a, b, c, d = rows[g:g + 4]
            ab = a + b
            abc = ab + c
            abcd = ab + (c + d)
            out += [total + a, total + ab, total + abc, total + abcd]
            total = out[-1]
        return out

    def plain(n, total):
        base = n * SPAN
        index, rows = load(base, BATCHES[0])
        for k, size in enumerate(BATCHES):
            now_index, now_rows = index, rows
            base += size
            if k + 1 < len(BATCHES):
                index, rows = load(base, BATCHES[k + 1])
            for i, value in zip(now_index, sums_of(total, now_rows)):
                grid_rows[pl.ds(i, 1), :] = value
                total = value
        return total

    def broken(n, total):
        def whole(group, bits, total):
            index, rows = load(group * BITS, BITS)
            rows = sums_of(total, rows)
            for u in range(BITS):
                grid_rows[pl.ds(index[u], 1), :] = rows[u]
            return rows[-1]

        def cut(group, bits, total):
            index, rows = load(group * BITS, BITS)
            for u in range(BITS):
                total = jnp.where(((bits >> u) & 1) == 1, rows[u], total + rows[u])
                rows[u] = total
            for u in range(BITS):
                grid_rows[pl.ds(index[u], 1), :] = rows[u]
            return total

        def sixteen(j, total):
            group = n * (SPAN // BITS) + j
            bits = starts[group]
            return lax.cond(bits == 0, whole, cut, group, bits, total)

        return lax.fori_loop(0, SPAN // BITS, sixteen, total)

    def walk(d, total):
        copy_order(d).wait()

        def span(n, total):
            return lax.cond(spans[0, n] == 0, plain, broken, n, total)

        return lax.fori_loop(d * piece_spans, (d + 1) * piece_spans, span, total)

    lax.fori_loop(0, group_size, walk, jnp.zeros((1, LANES), jnp.float32))

    block = lane_block((step_rows, LANES), fold)

    def merge(j, carry):
        d = owner(j)

        def step(k, carry):
            base, at = place(d, k)
            merged = grid_rows[pl.ds(at[0], step_rows), :]
            for q in range(1, fold):
                moved = pltpu.roll(grid_rows[pl.ds(at[q], step_rows), :], q * wide, 1)
                merged = jnp.where(block == q, moved, merged)
            stage[pl.ds(base, step_rows), :] = merged.astype(jnp.bfloat16)
            return carry

        carry = lax.fori_loop(0, part // step_rows, step, carry)
        for k in range(group_size):
            @pl.when(j == k)
            def _():
                copy_out(k, dsts[k]).start()
        return carry

    lax.fori_loop(0, group_size, merge, 0)
    for k in range(group_size):
        copy_out(k, dsts[k]).wait()


def solution(mesh):
    group_size = mesh.shape['group']

    def per_device(sort_keys, seg_ids, payload):
        rows_dev = sort_keys.shape[0]
        width = payload.shape[1]
        count = group_size * rows_dev
        tile = min(512, rows_dev // max(FOLDS))
        cols = [group_size * (LANES // fold) for fold in FOLDS]
        begin = [sum(cols[:c]) for c in range(len(FOLDS))]

        def estimate(c, flops):
            return pl.CostEstimate(flops=flops, bytes_accessed=4 * rows_dev * cols[c], transcendentals=0)

        def pack(c, rows):
            fold = FOLDS[c]
            part = rows_dev // fold
            return pl.pallas_call(
                functools.partial(pack_kernel, fold), name=f'pack{c}',
                out_shape=[jax.ShapeDtypeStruct((part, LANES), jnp.bfloat16)] * group_size,
                grid=(part // tile,),
                in_specs=[pl.BlockSpec(memory_space=pltpu.SMEM),
                          pl.BlockSpec((fold, tile, cols[c]), lambda i: (0, i, begin[c] // cols[c]))],
                out_specs=[pl.BlockSpec((tile, LANES), lambda i: (i, 0))] * group_size,
                scratch_shapes=[pltpu.VMEM((group_size, tile, LANES), jnp.bfloat16)],
                compiler_params=pltpu.CompilerParams(vmem_limit_bytes=60 * 2**20),
                cost_estimate=estimate(c, 50_000_000),
            )(place, rows.reshape(fold, part, width))

        def unpack(c, back, out):
            fold = FOLDS[c]
            part = rows_dev // fold
            first = out is None
            return pl.pallas_call(
                functools.partial(unpack_kernel, fold, group_size), name=f'unpack{c}',
                out_shape=jax.ShapeDtypeStruct((fold, part, width), jnp.bfloat16),
                grid=(part // tile,),
                in_specs=[pl.BlockSpec(memory_space=pltpu.SMEM)]
                + [pl.BlockSpec((tile, LANES), lambda i: (i, 0))] * group_size
                + ([] if first else [pl.BlockSpec(memory_space=pl.ANY)]),
                out_specs=pl.BlockSpec((fold, tile, cols[c]), lambda i: (0, i, begin[c] // cols[c])),
                scratch_shapes=[pltpu.VMEM((group_size, tile, LANES), jnp.bfloat16)],
                input_output_aliases={} if first else {1 + group_size: 0},
                compiler_params=pltpu.CompilerParams(vmem_limit_bytes=60 * 2**20),
                cost_estimate=estimate(c, 50_000_000),
            )(place, *back, *(() if first else (out.reshape(fold, part, width),))).reshape(rows_dev, width)

        def walk(c, order, starts, spans, rows):
            fold = FOLDS[c]
            return pl.pallas_call(
                functools.partial(walk_kernel, group_size, fold), name=f'walk{c}',
                out_shape=[jax.ShapeDtypeStruct((rows_dev // fold, LANES), jnp.bfloat16)] * group_size,
                in_specs=[pl.BlockSpec(memory_space=pltpu.SMEM), pl.BlockSpec(memory_space=pl.ANY)]
                + [pl.BlockSpec(memory_space=pltpu.SMEM)] * 2 + [pl.BlockSpec(memory_space=pl.ANY)] * group_size,
                out_specs=[pl.BlockSpec(memory_space=pl.ANY)] * group_size,
                scratch_shapes=[
                    pltpu.VMEM((count, LANES), jnp.float32),
                    pltpu.VMEM((count // fold, LANES), jnp.bfloat16),
                    pltpu.SMEM((count,), jnp.int32),
                    pltpu.SemaphoreType.DMA((group_size,)),
                    pltpu.SemaphoreType.DMA((group_size,)),
                    pltpu.SemaphoreType.DMA((group_size,)),
                ],
                compiler_params=pltpu.CompilerParams(vmem_limit_bytes=62 * 2**20),
                cost_estimate=estimate(c, 1_000_000_000),
            )(place, order, starts, spans, *rows)

        me = lax.axis_index('group')
        place = jnp.full((1,), me, jnp.int32)

        def shift(array, k):
            return lax.ppermute(array, 'group', [(i, (i + k) % group_size) for i in range(group_size)])

        halves = jnp.stack([sort_keys, (seg_ids >> 16).astype(jnp.float32), (seg_ids & 0xFFFF).astype(jnp.float32)])
        shifted = [halves] + [shift(halves, k) for k in range(1, group_size)]
        every = jnp.stack(shifted)
        owner = (me - jnp.arange(group_size, dtype=jnp.int32) + group_size) % group_size
        record = (owner[:, None] * rows_dev + jnp.arange(rows_dev, dtype=jnp.int32)[None, :]).reshape(count)
        keys = every[:, 0].reshape(count)
        ids = ((every[:, 1].astype(jnp.int32) << 16) | every[:, 2].astype(jnp.int32)).reshape(count)
        first = pack(0, payload)
        _, ids_sorted, order = lax.sort((keys, ids, record), num_keys=1, is_stable=False)
        new = jnp.concatenate([jnp.ones((1,), jnp.bool_), ids_sorted[1:] != ids_sorted[:-1]]).astype(jnp.int32)
        starts = jnp.sum(new.reshape(count // BITS, BITS) << jnp.arange(BITS, dtype=jnp.int32)[None, :], axis=1)
        spans = jnp.max(new.reshape(1, count // SPAN, SPAN), axis=2)
        order, starts, spans, folded = lax.optimization_barrier((order, starts, spans, payload))

        sent = [first] + [pack(c, folded) for c in range(1, len(FOLDS))]
        def forward(blocks):
            return [blocks[0]] + [shift(blocks[k], k) for k in range(1, group_size)]

        there = [forward(sent[0])]
        there[0], later = lax.optimization_barrier((there[0], sent[1:]))
        there += [forward(s) for s in later]
        done = [walk(c, order, starts, spans, t) for c, t in enumerate(there)]
        back = [[d[0]] + [shift(d[k], group_size - k) for k in range(1, group_size)] for d in done]
        out = None
        for c, b in enumerate(back):
            out = unpack(c, b, out)
        return out

    row_spec = P(('batch', 'group'))
    mat_spec = P(('batch', 'group'), None)
    return jax.shard_map(per_device, mesh=mesh, in_specs=(row_spec, row_spec, mat_spec),
                         out_specs=mat_spec, check_vma=False)
```

```python
import functools

import jax
import jax.numpy as jnp
from jax import lax
from jax.experimental import pallas as pl
from jax.experimental.pallas import tpu as pltpu
from jax.sharding import PartitionSpec as P


LANES = 128
FOLDS = (4, 4, 4)
PACK_STEP = 256
WALK_STEP = 1024
SUB = 8
SPAN = 128
BITS = 16


def lane_block(shape, fold):
    return lax.broadcasted_iota(jnp.int32, shape, 1) // (LANES // fold)


def swap_blocks(parts):
    fold = len(parts)
    wide = LANES // fold
    block = lane_block(parts[0].shape, fold)
    reach = 1
    while reach < fold:
        upper = (block // reach) % 2 == 1
        out = [None] * fold
        for k in range(fold):
            if (k // reach) % 2 == 0:
                a, b = parts[k], parts[k + reach]
                out[k] = jnp.where(upper, pltpu.roll(b, reach * wide, 1), a)
                out[k + reach] = jnp.where(upper, b, pltpu.roll(a, LANES - reach * wide, 1))
        parts = out
        reach *= 2
    return parts


def pack_kernel(fold, me, src, *refs):
    *outs, dst = refs
    step_rows = src.shape[1]

    def step(k, carry):
        rows = pl.ds(pl.multiple_of(k * PACK_STEP, PACK_STEP), PACK_STEP)
        for t in range(dst.shape[0] // fold):
            cols = slice(t * LANES, (t + 1) * LANES)
            parts = [src[q, rows, cols].astype(jnp.float32) for q in range(fold)]
            for l, part in enumerate(swap_blocks(parts)):
                dst[t * fold + l, rows, :] = part.astype(jnp.bfloat16)
        return carry

    lax.fori_loop(0, step_rows // PACK_STEP, step, 0)
    for k, out in enumerate(outs):
        out[...] = dst[lax.rem(me[0] + k, len(outs))]


def unpack_kernel(fold, group_size, me, *refs):
    dst, src = refs[-2:]
    for k in range(group_size):
        src[lax.rem(me[0] + k, group_size)] = refs[k][...]
    step_rows = src.shape[1]

    def step(k, carry):
        rows = pl.ds(pl.multiple_of(k * PACK_STEP, PACK_STEP), PACK_STEP)
        for t in range(src.shape[0] // fold):
            cols = slice(t * LANES, (t + 1) * LANES)
            parts = [src[t * fold + l, rows, :].astype(jnp.float32) for l in range(fold)]
            for q, part in enumerate(swap_blocks(parts)):
                dst[q, rows, cols] = part.astype(jnp.bfloat16)
        return carry

    lax.fori_loop(0, step_rows // PACK_STEP, step, 0)


def walk_kernel(group_size, fold, me, order_hbm, starts, spans, *refs):
    srcs, dsts = refs[:group_size], refs[group_size:2 * group_size]
    grid_rows, stage, order, in_sem, out_sem, order_sem = refs[2 * group_size:]
    packed_rows = stage.shape[0]
    part = packed_rows // group_size
    step_rows = min(WALK_STEP, part)
    wide = LANES // fold
    piece = order.shape[0] // group_size
    piece_spans = piece // SPAN

    def part_rows(d):
        return pl.ds(pl.multiple_of(d * part, part), part)

    def owner(k):
        return lax.rem(me[0] - k + group_size, group_size)

    def copy_in(k, src):
        return pltpu.make_async_copy(src, stage.at[part_rows(owner(k))], in_sem.at[k])

    def copy_out(k, dst):
        return pltpu.make_async_copy(stage.at[part_rows(owner(k))], dst, out_sem.at[k])

    def copy_order(d):
        rows = pl.ds(pl.multiple_of(d * piece, piece), piece)
        return pltpu.make_async_copy(order_hbm.at[rows], order.at[rows], order_sem.at[d])

    for k in range(group_size):
        copy_in(k, srcs[k]).start()
    for d in range(group_size):
        copy_order(d).start()

    def place(d, k):
        base = pl.multiple_of(d * part + k * step_rows, step_rows)
        return base, [pl.multiple_of((d * fold + q) * part + k * step_rows, step_rows) for q in range(fold)]

    def spread(j, carry):
        copy_in(j, srcs[0]).wait()
        d = owner(j)

        def step(k, carry):
            base, at = place(d, k)
            data = stage[pl.ds(base, step_rows), :].astype(jnp.float32)
            for q in range(fold):
                grid_rows[pl.ds(at[q], step_rows), :] = data if q == 0 else pltpu.roll(data, LANES - q * wide, 1)
            return carry

        return lax.fori_loop(0, part // step_rows, step, carry)

    lax.fori_loop(0, group_size, spread, 0)

    def load(base, rows):
        index = [order[base + u] for u in range(rows)]
        return index, [grid_rows[pl.ds(i, 1), :] for i in index]

    def sums_of(total, rows):
        out = []
        for g in range(0, len(rows), 4):
            a, b, c, d = rows[g:g + 4]
            ab = a + b
            abc = ab + c
            abcd = ab + (c + d)
            out += [total + a, total + ab, total + abc, total + abcd]
            total = out[-1]
        return out

    def plain(n, total):
        base = n * SPAN
        index, rows = load(base, SUB)
        for k in range(SPAN // SUB):
            now_index, now_rows = index, rows
            if k + 1 < SPAN // SUB:
                index, rows = load(base + (k + 1) * SUB, SUB)
            for i, value in zip(now_index, sums_of(total, now_rows)):
                grid_rows[pl.ds(i, 1), :] = value
                total = value
        return total

    def broken(n, total):
        def whole(group, bits, total):
            index, rows = load(group * BITS, BITS)
            rows = sums_of(total, rows)
            for u in range(BITS):
                grid_rows[pl.ds(index[u], 1), :] = rows[u]
            return rows[-1]

        def cut(group, bits, total):
            index, rows = load(group * BITS, BITS)
            for u in range(BITS):
                total = jnp.where(((bits >> u) & 1) == 1, rows[u], total + rows[u])
                rows[u] = total
            for u in range(BITS):
                grid_rows[pl.ds(index[u], 1), :] = rows[u]
            return total

        def sixteen(j, total):
            group = n * (SPAN // BITS) + j
            bits = starts[group]
            return lax.cond(bits == 0, whole, cut, group, bits, total)

        return lax.fori_loop(0, SPAN // BITS, sixteen, total)

    def walk(d, total):
        copy_order(d).wait()

        def span(n, total):
            return lax.cond(spans[0, n] == 0, plain, broken, n, total)

        return lax.fori_loop(d * piece_spans, (d + 1) * piece_spans, span, total)

    lax.fori_loop(0, group_size, walk, jnp.zeros((1, LANES), jnp.float32))

    block = lane_block((step_rows, LANES), fold)

    def merge(j, carry):
        d = owner(j)

        def step(k, carry):
            base, at = place(d, k)
            merged = grid_rows[pl.ds(at[0], step_rows), :]
            for q in range(1, fold):
                moved = pltpu.roll(grid_rows[pl.ds(at[q], step_rows), :], q * wide, 1)
                merged = jnp.where(block == q, moved, merged)
            stage[pl.ds(base, step_rows), :] = merged.astype(jnp.bfloat16)
            return carry

        carry = lax.fori_loop(0, part // step_rows, step, carry)
        for k in range(group_size):
            @pl.when(j == k)
            def _():
                copy_out(k, dsts[k]).start()
        return carry

    lax.fori_loop(0, group_size, merge, 0)
    for k in range(group_size):
        copy_out(k, dsts[k]).wait()


def solution(mesh):
    group_size = mesh.shape['group']

    def per_device(sort_keys, seg_ids, payload):
        rows_dev = sort_keys.shape[0]
        width = payload.shape[1]
        count = group_size * rows_dev
        tile = min(512, rows_dev // max(FOLDS))
        cols = [group_size * (LANES // fold) for fold in FOLDS]
        begin = [sum(cols[:c]) for c in range(len(FOLDS))]

        def estimate(c, flops):
            return pl.CostEstimate(flops=flops, bytes_accessed=4 * rows_dev * cols[c], transcendentals=0)

        def pack(c, rows):
            fold = FOLDS[c]
            part = rows_dev // fold
            return pl.pallas_call(
                functools.partial(pack_kernel, fold), name=f'pack{c}',
                out_shape=[jax.ShapeDtypeStruct((part, LANES), jnp.bfloat16)] * group_size,
                grid=(part // tile,),
                in_specs=[pl.BlockSpec(memory_space=pltpu.SMEM),
                          pl.BlockSpec((fold, tile, cols[c]), lambda i: (0, i, begin[c] // cols[c]))],
                out_specs=[pl.BlockSpec((tile, LANES), lambda i: (i, 0))] * group_size,
                scratch_shapes=[pltpu.VMEM((group_size, tile, LANES), jnp.bfloat16)],
                compiler_params=pltpu.CompilerParams(vmem_limit_bytes=60 * 2**20),
                cost_estimate=estimate(c, 50_000_000),
            )(place, rows.reshape(fold, part, width))

        def unpack(c, back, out):
            fold = FOLDS[c]
            part = rows_dev // fold
            first = out is None
            return pl.pallas_call(
                functools.partial(unpack_kernel, fold, group_size), name=f'unpack{c}',
                out_shape=jax.ShapeDtypeStruct((fold, part, width), jnp.bfloat16),
                grid=(part // tile,),
                in_specs=[pl.BlockSpec(memory_space=pltpu.SMEM)]
                + [pl.BlockSpec((tile, LANES), lambda i: (i, 0))] * group_size
                + ([] if first else [pl.BlockSpec(memory_space=pl.ANY)]),
                out_specs=pl.BlockSpec((fold, tile, cols[c]), lambda i: (0, i, begin[c] // cols[c])),
                scratch_shapes=[pltpu.VMEM((group_size, tile, LANES), jnp.bfloat16)],
                input_output_aliases={} if first else {1 + group_size: 0},
                compiler_params=pltpu.CompilerParams(vmem_limit_bytes=60 * 2**20),
                cost_estimate=estimate(c, 50_000_000),
            )(place, *back, *(() if first else (out.reshape(fold, part, width),))).reshape(rows_dev, width)

        def walk(c, order, starts, spans, rows):
            fold = FOLDS[c]
            return pl.pallas_call(
                functools.partial(walk_kernel, group_size, fold), name=f'walk{c}',
                out_shape=[jax.ShapeDtypeStruct((rows_dev // fold, LANES), jnp.bfloat16)] * group_size,
                in_specs=[pl.BlockSpec(memory_space=pltpu.SMEM), pl.BlockSpec(memory_space=pl.ANY)]
                + [pl.BlockSpec(memory_space=pltpu.SMEM)] * 2 + [pl.BlockSpec(memory_space=pl.ANY)] * group_size,
                out_specs=[pl.BlockSpec(memory_space=pl.ANY)] * group_size,
                scratch_shapes=[
                    pltpu.VMEM((count, LANES), jnp.float32),
                    pltpu.VMEM((count // fold, LANES), jnp.bfloat16),
                    pltpu.SMEM((count,), jnp.int32),
                    pltpu.SemaphoreType.DMA((group_size,)),
                    pltpu.SemaphoreType.DMA((group_size,)),
                    pltpu.SemaphoreType.DMA((group_size,)),
                ],
                compiler_params=pltpu.CompilerParams(vmem_limit_bytes=62 * 2**20),
                cost_estimate=estimate(c, 1_000_000_000),
            )(place, order, starts, spans, *rows)

        me = lax.axis_index('group')
        place = jnp.full((1,), me, jnp.int32)

        def shift(array, k):
            return lax.ppermute(array, 'group', [(i, (i + k) % group_size) for i in range(group_size)])

        halves = jnp.stack([sort_keys, (seg_ids >> 16).astype(jnp.float32), (seg_ids & 0xFFFF).astype(jnp.float32)])
        shifted = [halves] + [shift(halves, k) for k in range(1, group_size)]
        first = pack(0, payload)
        shifted, first = lax.optimization_barrier((shifted, first))
        every = jnp.stack(shifted)
        owner = (me - jnp.arange(group_size, dtype=jnp.int32) + group_size) % group_size
        record = (owner[:, None] * rows_dev + jnp.arange(rows_dev, dtype=jnp.int32)[None, :]).reshape(count)
        keys = every[:, 0].reshape(count)
        ids = ((every[:, 1].astype(jnp.int32) << 16) | every[:, 2].astype(jnp.int32)).reshape(count)
        _, ids_sorted, order = lax.sort((keys, ids, record), num_keys=1, is_stable=False)
        new = jnp.concatenate([jnp.ones((1,), jnp.bool_), ids_sorted[1:] != ids_sorted[:-1]]).astype(jnp.int32)
        starts = jnp.sum(new.reshape(count // BITS, BITS) << jnp.arange(BITS, dtype=jnp.int32)[None, :], axis=1)
        spans = jnp.max(new.reshape(1, count // SPAN, SPAN), axis=2)
        order, starts, spans, folded = lax.optimization_barrier((order, starts, spans, payload))

        sent = [first] + [pack(c, folded) for c in range(1, len(FOLDS))]
        sent[1:] = lax.optimization_barrier(sent[1:])
        there = [[s[0]] + [shift(s[k], k) for k in range(1, group_size)] for s in sent]
        done = [walk(c, order, starts, spans, t) for c, t in enumerate(there)]
        back = [[d[0]] + [shift(d[k], group_size - k) for k in range(1, group_size)] for d in done]
        out = None
        for c, b in enumerate(back):
            out = unpack(c, b, out)
        return out

    row_spec = P(('batch', 'group'))
    mat_spec = P(('batch', 'group'), None)
    return jax.shard_map(per_device, mesh=mesh, in_specs=(row_spec, row_spec, mat_spec),
                         out_specs=mat_spec, check_vma=False)
```

```python
import functools

import jax
import jax.numpy as jnp
from jax import lax
from jax.experimental import pallas as pl
from jax.experimental.pallas import tpu as pltpu
from jax.sharding import PartitionSpec as P


LANES = 128
FOLDS = (4, 4, 4)
PACK_STEP = 256
WALK_STEP = 1024
SUB = 8
SPAN = 256
HALF = SPAN // 2
BITS = 16


def lane_block(shape, fold):
    return lax.broadcasted_iota(jnp.int32, shape, 1) // (LANES // fold)


def swap_blocks(parts):
    fold = len(parts)
    wide = LANES // fold
    block = lane_block(parts[0].shape, fold)
    reach = 1
    while reach < fold:
        upper = (block // reach) % 2 == 1
        out = [None] * fold
        for k in range(fold):
            if (k // reach) % 2 == 0:
                a, b = parts[k], parts[k + reach]
                out[k] = jnp.where(upper, pltpu.roll(b, reach * wide, 1), a)
                out[k + reach] = jnp.where(upper, b, pltpu.roll(a, LANES - reach * wide, 1))
        parts = out
        reach *= 2
    return parts


def pack_kernel(fold, me, src, *refs):
    *outs, dst = refs
    step_rows = src.shape[1]

    def step(k, carry):
        rows = pl.ds(pl.multiple_of(k * PACK_STEP, PACK_STEP), PACK_STEP)
        for t in range(dst.shape[0] // fold):
            cols = slice(t * LANES, (t + 1) * LANES)
            parts = [src[q, rows, cols].astype(jnp.float32) for q in range(fold)]
            for l, part in enumerate(swap_blocks(parts)):
                dst[t * fold + l, rows, :] = part.astype(jnp.bfloat16)
        return carry

    lax.fori_loop(0, step_rows // PACK_STEP, step, 0)
    for k, out in enumerate(outs):
        out[...] = dst[lax.rem(me[0] + k, len(outs))]


def unpack_kernel(fold, group_size, me, *refs):
    dst, src = refs[-2:]
    for k in range(group_size):
        src[lax.rem(me[0] + k, group_size)] = refs[k][...]
    step_rows = src.shape[1]

    def step(k, carry):
        rows = pl.ds(pl.multiple_of(k * PACK_STEP, PACK_STEP), PACK_STEP)
        for t in range(src.shape[0] // fold):
            cols = slice(t * LANES, (t + 1) * LANES)
            parts = [src[t * fold + l, rows, :].astype(jnp.float32) for l in range(fold)]
            for q, part in enumerate(swap_blocks(parts)):
                dst[q, rows, cols] = part.astype(jnp.bfloat16)
        return carry

    lax.fori_loop(0, step_rows // PACK_STEP, step, 0)


def walk_kernel(group_size, fold, me, order_hbm, starts, spans, *refs):
    srcs, dsts = refs[:group_size], refs[group_size:2 * group_size]
    grid_rows, stage, order, in_sem, out_sem, order_sem = refs[2 * group_size:]
    packed_rows = stage.shape[0]
    part = packed_rows // group_size
    step_rows = min(WALK_STEP, part)
    wide = LANES // fold
    piece = order.shape[0] // group_size
    piece_spans = piece // SPAN

    def part_rows(d):
        return pl.ds(pl.multiple_of(d * part, part), part)

    def owner(k):
        return lax.rem(me[0] - k + group_size, group_size)

    def copy_in(k, src):
        return pltpu.make_async_copy(src, stage.at[part_rows(owner(k))], in_sem.at[k])

    def copy_out(k, dst):
        return pltpu.make_async_copy(stage.at[part_rows(owner(k))], dst, out_sem.at[k])

    def copy_order(d):
        rows = pl.ds(pl.multiple_of(d * piece, piece), piece)
        return pltpu.make_async_copy(order_hbm.at[rows], order.at[rows], order_sem.at[d])

    for k in range(group_size):
        copy_in(k, srcs[k]).start()
    for d in range(group_size):
        copy_order(d).start()

    def place(d, k):
        base = pl.multiple_of(d * part + k * step_rows, step_rows)
        return base, [pl.multiple_of((d * fold + q) * part + k * step_rows, step_rows) for q in range(fold)]

    def spread(j, carry):
        copy_in(j, srcs[0]).wait()
        d = owner(j)

        def step(k, carry):
            base, at = place(d, k)
            data = stage[pl.ds(base, step_rows), :]
            for q in range(fold):
                moved = data if q == 0 else pltpu.roll(data, LANES - q * wide, 1)
                grid_rows[pl.ds(at[q], step_rows), :] = moved.astype(jnp.float32)
            return carry

        return lax.fori_loop(0, part // step_rows, step, carry)

    lax.fori_loop(0, group_size, spread, 0)

    def load(base, rows):
        index = [order[base + u] for u in range(rows)]
        return index, [grid_rows[pl.ds(i, 1), :] for i in index]

    def sums_of(total, rows):
        out = []
        for g in range(0, len(rows), 4):
            a, b, c, d = rows[g:g + 4]
            ab = a + b
            abc = ab + c
            abcd = ab + (c + d)
            out += [total + a, total + ab, total + abc, total + abcd]
            total = out[-1]
        return out

    def straight(base, size, total):
        index, rows = load(base, SUB)
        for k in range(size // SUB):
            now_index, now_rows = index, rows
            if k + 1 < size // SUB:
                index, rows = load(base + (k + 1) * SUB, SUB)
            for i, value in zip(now_index, sums_of(total, now_rows)):
                grid_rows[pl.ds(i, 1), :] = value
                total = value
        return total

    def plain(n, total):
        return straight(n * SPAN, SPAN, total)

    def broken(n, total):
        def whole(group, bits, total):
            index, rows = load(group * BITS, BITS)
            rows = sums_of(total, rows)
            for u in range(BITS):
                grid_rows[pl.ds(index[u], 1), :] = rows[u]
            return rows[-1]

        def cut(group, bits, total):
            index, rows = load(group * BITS, BITS)
            for u in range(BITS):
                total = jnp.where(((bits >> u) & 1) == 1, rows[u], total + rows[u])
                rows[u] = total
            for u in range(BITS):
                grid_rows[pl.ds(index[u], 1), :] = rows[u]
            return total

        def half(h, total):
            first = (n * SPAN + h * HALF) // BITS
            any_start = starts[first]
            for j in range(1, HALF // BITS):
                any_start = any_start | starts[first + j]

            def sixteen(j, total):
                bits = starts[first + j]
                return lax.cond(bits == 0, whole, cut, first + j, bits, total)

            return lax.cond(any_start == 0, lambda total: straight(n * SPAN + h * HALF, HALF, total),
                            lambda total: lax.fori_loop(0, HALF // BITS, sixteen, total), total)

        return lax.fori_loop(0, SPAN // HALF, half, total)

    def walk(d, total):
        copy_order(d).wait()

        def span(n, total):
            return lax.cond(spans[0, n] == 0, plain, broken, n, total)

        return lax.fori_loop(d * piece_spans, (d + 1) * piece_spans, span, total)

    lax.fori_loop(0, group_size, walk, jnp.zeros((1, LANES), jnp.float32))

    block = lane_block((step_rows, LANES), fold)

    def merge(j, carry):
        d = owner(j)

        def step(k, carry):
            base, at = place(d, k)
            merged = grid_rows[pl.ds(at[0], step_rows), :].astype(jnp.bfloat16)
            for q in range(1, fold):
                moved = pltpu.roll(grid_rows[pl.ds(at[q], step_rows), :].astype(jnp.bfloat16), q * wide, 1)
                merged = jnp.where(block == q, moved, merged)
            stage[pl.ds(base, step_rows), :] = merged
            return carry

        carry = lax.fori_loop(0, part // step_rows, step, carry)
        for k in range(group_size):
            @pl.when(j == k)
            def _():
                copy_out(k, dsts[k]).start()
        return carry

    lax.fori_loop(0, group_size, merge, 0)
    for k in range(group_size):
        copy_out(k, dsts[k]).wait()


def solution(mesh):
    group_size = mesh.shape['group']

    def per_device(sort_keys, seg_ids, payload):
        rows_dev = sort_keys.shape[0]
        width = payload.shape[1]
        count = group_size * rows_dev
        tile = min(512, rows_dev // max(FOLDS))
        cols = [group_size * (LANES // fold) for fold in FOLDS]
        begin = [sum(cols[:c]) for c in range(len(FOLDS))]

        def estimate(c, flops):
            return pl.CostEstimate(flops=flops, bytes_accessed=4 * rows_dev * cols[c], transcendentals=0)

        def pack(c, rows):
            fold = FOLDS[c]
            part = rows_dev // fold
            return pl.pallas_call(
                functools.partial(pack_kernel, fold), name=f'pack{c}',
                out_shape=[jax.ShapeDtypeStruct((part, LANES), jnp.bfloat16)] * group_size,
                grid=(part // tile,),
                in_specs=[pl.BlockSpec(memory_space=pltpu.SMEM),
                          pl.BlockSpec((fold, tile, cols[c]), lambda i: (0, i, begin[c] // cols[c]))],
                out_specs=[pl.BlockSpec((tile, LANES), lambda i: (i, 0))] * group_size,
                scratch_shapes=[pltpu.VMEM((group_size, tile, LANES), jnp.bfloat16)],
                compiler_params=pltpu.CompilerParams(vmem_limit_bytes=60 * 2**20),
                cost_estimate=estimate(c, 50_000_000),
            )(place, rows.reshape(fold, part, width))

        def unpack(c, back, out):
            fold = FOLDS[c]
            part = rows_dev // fold
            first = out is None
            return pl.pallas_call(
                functools.partial(unpack_kernel, fold, group_size), name=f'unpack{c}',
                out_shape=jax.ShapeDtypeStruct((fold, part, width), jnp.bfloat16),
                grid=(part // tile,),
                in_specs=[pl.BlockSpec(memory_space=pltpu.SMEM)]
                + [pl.BlockSpec((tile, LANES), lambda i: (i, 0))] * group_size
                + ([] if first else [pl.BlockSpec(memory_space=pl.ANY)]),
                out_specs=pl.BlockSpec((fold, tile, cols[c]), lambda i: (0, i, begin[c] // cols[c])),
                scratch_shapes=[pltpu.VMEM((group_size, tile, LANES), jnp.bfloat16)],
                input_output_aliases={} if first else {1 + group_size: 0},
                compiler_params=pltpu.CompilerParams(vmem_limit_bytes=60 * 2**20),
                cost_estimate=estimate(c, 50_000_000),
            )(place, *back, *(() if first else (out.reshape(fold, part, width),))).reshape(rows_dev, width)

        def walk(c, order, starts, spans, rows):
            fold = FOLDS[c]
            return pl.pallas_call(
                functools.partial(walk_kernel, group_size, fold), name=f'walk{c}',
                out_shape=[jax.ShapeDtypeStruct((rows_dev // fold, LANES), jnp.bfloat16)] * group_size,
                in_specs=[pl.BlockSpec(memory_space=pltpu.SMEM), pl.BlockSpec(memory_space=pl.ANY)]
                + [pl.BlockSpec(memory_space=pltpu.SMEM)] * 2 + [pl.BlockSpec(memory_space=pl.ANY)] * group_size,
                out_specs=[pl.BlockSpec(memory_space=pl.ANY)] * group_size,
                scratch_shapes=[
                    pltpu.VMEM((count, LANES), jnp.float32),
                    pltpu.VMEM((count // fold, LANES), jnp.bfloat16),
                    pltpu.SMEM((count,), jnp.int32),
                    pltpu.SemaphoreType.DMA((group_size,)),
                    pltpu.SemaphoreType.DMA((group_size,)),
                    pltpu.SemaphoreType.DMA((group_size,)),
                ],
                compiler_params=pltpu.CompilerParams(vmem_limit_bytes=62 * 2**20),
                cost_estimate=estimate(c, 1_000_000_000),
            )(place, order, starts, spans, *rows)

        me = lax.axis_index('group')
        place = jnp.full((1,), me, jnp.int32)

        def shift(array, k):
            return lax.ppermute(array, 'group', [(i, (i + k) % group_size) for i in range(group_size)])

        halves = jnp.stack([sort_keys, (seg_ids >> 16).astype(jnp.float32), (seg_ids & 0xFFFF).astype(jnp.float32)])
        shifted = [halves] + [shift(halves, k) for k in range(1, group_size)]
        every = jnp.stack(shifted)
        owner = (me - jnp.arange(group_size, dtype=jnp.int32) + group_size) % group_size
        record = (owner[:, None] * rows_dev + jnp.arange(rows_dev, dtype=jnp.int32)[None, :]).reshape(count)
        keys = every[:, 0].reshape(count)
        ids = ((every[:, 1].astype(jnp.int32) << 16) | every[:, 2].astype(jnp.int32)).reshape(count)
        first = pack(0, payload)
        _, ids_sorted, order = lax.sort((keys, ids, record), num_keys=1, is_stable=False)
        new = jnp.concatenate([jnp.ones((1,), jnp.bool_), ids_sorted[1:] != ids_sorted[:-1]]).astype(jnp.int32)
        starts = jnp.sum(new.reshape(count // BITS, BITS) << jnp.arange(BITS, dtype=jnp.int32)[None, :], axis=1)
        spans = jnp.max(new.reshape(1, count // SPAN, SPAN), axis=2)
        order, starts, spans, folded = lax.optimization_barrier((order, starts, spans, payload))

        sent = [first] + [pack(c, folded) for c in range(1, len(FOLDS))]
        there = [[s[0]] + [shift(s[k], k) for k in range(1, group_size)] for s in sent]
        done = [walk(c, order, starts, spans, t) for c, t in enumerate(there)]
        back = [[d[0]] + [shift(d[k], group_size - k) for k in range(1, group_size)] for d in done]
        out = None
        for c, b in enumerate(back):
            out = unpack(c, b, out)
        return out

    row_spec = P(('batch', 'group'))
    mat_spec = P(('batch', 'group'), None)
    return jax.shard_map(per_device, mesh=mesh, in_specs=(row_spec, row_spec, mat_spec),
                         out_specs=mat_spec, check_vma=False)
```

```python
import functools

import jax
import jax.numpy as jnp
from jax import lax
from jax.experimental import pallas as pl
from jax.experimental.pallas import tpu as pltpu
from jax.sharding import PartitionSpec as P


LANES = 128
FOLDS = (4, 4, 4)
PACK_STEP = 256
WALK_STEPS = (1024, 256, 1024)
SUB = 8
SPAN = 256
HALF = SPAN // 2
BITS = 16


def lane_block(shape, fold):
    return lax.broadcasted_iota(jnp.int32, shape, 1) // (LANES // fold)


def swap_blocks(parts):
    fold = len(parts)
    wide = LANES // fold
    block = lane_block(parts[0].shape, fold)
    reach = 1
    while reach < fold:
        upper = (block // reach) % 2 == 1
        out = [None] * fold
        for k in range(fold):
            if (k // reach) % 2 == 0:
                a, b = parts[k], parts[k + reach]
                out[k] = jnp.where(upper, pltpu.roll(b, reach * wide, 1), a)
                out[k + reach] = jnp.where(upper, b, pltpu.roll(a, LANES - reach * wide, 1))
        parts = out
        reach *= 2
    return parts


def pack_kernel(fold, me, src, *refs):
    *outs, dst = refs
    step_rows = src.shape[1]

    def step(k, carry):
        rows = pl.ds(pl.multiple_of(k * PACK_STEP, PACK_STEP), PACK_STEP)
        for t in range(dst.shape[0] // fold):
            cols = slice(t * LANES, (t + 1) * LANES)
            parts = [src[q, rows, cols].astype(jnp.float32) for q in range(fold)]
            for l, part in enumerate(swap_blocks(parts)):
                dst[t * fold + l, rows, :] = part.astype(jnp.bfloat16)
        return carry

    lax.fori_loop(0, step_rows // PACK_STEP, step, 0)
    for k, out in enumerate(outs):
        out[...] = dst[lax.rem(me[0] + k, len(outs))]


def unpack_kernel(fold, group_size, me, *refs):
    dst, src = refs[-2:]
    for k in range(group_size):
        src[lax.rem(me[0] + k, group_size)] = refs[k][...]
    step_rows = src.shape[1]

    def step(k, carry):
        rows = pl.ds(pl.multiple_of(k * PACK_STEP, PACK_STEP), PACK_STEP)
        for t in range(src.shape[0] // fold):
            cols = slice(t * LANES, (t + 1) * LANES)
            parts = [src[t * fold + l, rows, :].astype(jnp.float32) for l in range(fold)]
            for q, part in enumerate(swap_blocks(parts)):
                dst[q, rows, cols] = part.astype(jnp.bfloat16)
        return carry

    lax.fori_loop(0, step_rows // PACK_STEP, step, 0)


def walk_kernel(group_size, fold, most_rows, me, order_hbm, starts, spans, *refs):
    srcs, dsts = refs[:group_size], refs[group_size:2 * group_size]
    grid_rows, stage, order, in_sem, out_sem, order_sem = refs[2 * group_size:]
    packed_rows = stage.shape[0]
    part = packed_rows // group_size
    step_rows = min(most_rows, part)
    wide = LANES // fold
    piece = order.shape[0] // group_size
    piece_spans = piece // SPAN

    def part_rows(d):
        return pl.ds(pl.multiple_of(d * part, part), part)

    def owner(k):
        return lax.rem(me[0] - k + group_size, group_size)

    def copy_in(k, src):
        return pltpu.make_async_copy(src, stage.at[part_rows(owner(k))], in_sem.at[k])

    def copy_out(k, dst):
        return pltpu.make_async_copy(stage.at[part_rows(owner(k))], dst, out_sem.at[k])

    def copy_order(d):
        rows = pl.ds(pl.multiple_of(d * piece, piece), piece)
        return pltpu.make_async_copy(order_hbm.at[rows], order.at[rows], order_sem.at[d])

    for k in range(group_size):
        copy_in(k, srcs[k]).start()
    for d in range(group_size):
        copy_order(d).start()

    def place(d, k):
        base = pl.multiple_of(d * part + k * step_rows, step_rows)
        return base, [pl.multiple_of((d * fold + q) * part + k * step_rows, step_rows) for q in range(fold)]

    def spread(j, carry):
        copy_in(j, srcs[0]).wait()
        d = owner(j)

        def step(k, carry):
            base, at = place(d, k)
            data = stage[pl.ds(base, step_rows), :]
            for q in range(fold):
                moved = data if q == 0 else pltpu.roll(data, LANES - q * wide, 1)
                grid_rows[pl.ds(at[q], step_rows), :] = moved.astype(jnp.float32)
            return carry

        return lax.fori_loop(0, part // step_rows, step, carry)

    lax.fori_loop(0, group_size, spread, 0)

    def load(base, rows):
        index = [order[base + u] for u in range(rows)]
        return index, [grid_rows[pl.ds(i, 1), :] for i in index]

    def sums_of(total, rows):
        out = []
        for g in range(0, len(rows), 4):
            a, b, c, d = rows[g:g + 4]
            ab = a + b
            abc = ab + c
            abcd = ab + (c + d)
            out += [total + a, total + ab, total + abc, total + abcd]
            total = out[-1]
        return out

    def straight(base, size, total):
        index, rows = load(base, SUB)
        for k in range(size // SUB):
            now_index, now_rows = index, rows
            if k + 1 < size // SUB:
                index, rows = load(base + (k + 1) * SUB, SUB)
            for i, value in zip(now_index, sums_of(total, now_rows)):
                grid_rows[pl.ds(i, 1), :] = value
                total = value
        return total

    def plain(n, total):
        return straight(n * SPAN, SPAN, total)

    def broken(n, total):
        def whole(group, bits, total):
            index, rows = load(group * BITS, BITS)
            rows = sums_of(total, rows)
            for u in range(BITS):
                grid_rows[pl.ds(index[u], 1), :] = rows[u]
            return rows[-1]

        def cut(group, bits, total):
            index, rows = load(group * BITS, BITS)
            for u in range(BITS):
                total = jnp.where(((bits >> u) & 1) == 1, rows[u], total + rows[u])
                rows[u] = total
            for u in range(BITS):
                grid_rows[pl.ds(index[u], 1), :] = rows[u]
            return total

        def half(h, total):
            first = (n * SPAN + h * HALF) // BITS
            any_start = starts[first]
            for j in range(1, HALF // BITS):
                any_start = any_start | starts[first + j]

            def sixteen(j, total):
                bits = starts[first + j]
                return lax.cond(bits == 0, whole, cut, first + j, bits, total)

            return lax.cond(any_start == 0, lambda total: straight(n * SPAN + h * HALF, HALF, total),
                            lambda total: lax.fori_loop(0, HALF // BITS, sixteen, total), total)

        return lax.fori_loop(0, SPAN // HALF, half, total)

    def walk(d, total):
        copy_order(d).wait()

        def span(n, total):
            return lax.cond(spans[0, n] == 0, plain, broken, n, total)

        return lax.fori_loop(d * piece_spans, (d + 1) * piece_spans, span, total)

    lax.fori_loop(0, group_size, walk, jnp.zeros((1, LANES), jnp.float32))

    block = lane_block((step_rows, LANES), fold)

    def merge(j, carry):
        d = owner(j)

        def step(k, carry):
            base, at = place(d, k)
            merged = grid_rows[pl.ds(at[0], step_rows), :].astype(jnp.bfloat16)
            for q in range(1, fold):
                moved = pltpu.roll(grid_rows[pl.ds(at[q], step_rows), :].astype(jnp.bfloat16), q * wide, 1)
                merged = jnp.where(block == q, moved, merged)
            stage[pl.ds(base, step_rows), :] = merged
            return carry

        carry = lax.fori_loop(0, part // step_rows, step, carry)
        for k in range(group_size):
            @pl.when(j == k)
            def _():
                copy_out(k, dsts[k]).start()
        return carry

    lax.fori_loop(0, group_size, merge, 0)
    for k in range(group_size):
        copy_out(k, dsts[k]).wait()


def solution(mesh):
    group_size = mesh.shape['group']

    def per_device(sort_keys, seg_ids, payload):
        rows_dev = sort_keys.shape[0]
        width = payload.shape[1]
        count = group_size * rows_dev
        tile = min(512, rows_dev // max(FOLDS))
        cols = [group_size * (LANES // fold) for fold in FOLDS]
        begin = [sum(cols[:c]) for c in range(len(FOLDS))]

        def estimate(c, flops):
            return pl.CostEstimate(flops=flops, bytes_accessed=4 * rows_dev * cols[c], transcendentals=0)

        def pack(c, rows):
            fold = FOLDS[c]
            part = rows_dev // fold
            return pl.pallas_call(
                functools.partial(pack_kernel, fold), name=f'pack{c}',
                out_shape=[jax.ShapeDtypeStruct((part, LANES), jnp.bfloat16)] * group_size,
                grid=(part // tile,),
                in_specs=[pl.BlockSpec(memory_space=pltpu.SMEM),
                          pl.BlockSpec((fold, tile, cols[c]), lambda i: (0, i, begin[c] // cols[c]))],
                out_specs=[pl.BlockSpec((tile, LANES), lambda i: (i, 0))] * group_size,
                scratch_shapes=[pltpu.VMEM((group_size, tile, LANES), jnp.bfloat16)],
                compiler_params=pltpu.CompilerParams(vmem_limit_bytes=60 * 2**20),
                cost_estimate=estimate(c, 50_000_000),
            )(place, rows.reshape(fold, part, width))

        def unpack(c, back, out):
            fold = FOLDS[c]
            part = rows_dev // fold
            first = out is None
            return pl.pallas_call(
                functools.partial(unpack_kernel, fold, group_size), name=f'unpack{c}',
                out_shape=jax.ShapeDtypeStruct((fold, part, width), jnp.bfloat16),
                grid=(part // tile,),
                in_specs=[pl.BlockSpec(memory_space=pltpu.SMEM)]
                + [pl.BlockSpec((tile, LANES), lambda i: (i, 0))] * group_size
                + ([] if first else [pl.BlockSpec(memory_space=pl.ANY)]),
                out_specs=pl.BlockSpec((fold, tile, cols[c]), lambda i: (0, i, begin[c] // cols[c])),
                scratch_shapes=[pltpu.VMEM((group_size, tile, LANES), jnp.bfloat16)],
                input_output_aliases={} if first else {1 + group_size: 0},
                compiler_params=pltpu.CompilerParams(vmem_limit_bytes=60 * 2**20),
                cost_estimate=estimate(c, 50_000_000),
            )(place, *back, *(() if first else (out.reshape(fold, part, width),))).reshape(rows_dev, width)

        def walk(c, order, starts, spans, rows):
            fold = FOLDS[c]
            return pl.pallas_call(
                functools.partial(walk_kernel, group_size, fold, WALK_STEPS[c]), name=f'walk{c}',
                out_shape=[jax.ShapeDtypeStruct((rows_dev // fold, LANES), jnp.bfloat16)] * group_size,
                in_specs=[pl.BlockSpec(memory_space=pltpu.SMEM), pl.BlockSpec(memory_space=pl.ANY)]
                + [pl.BlockSpec(memory_space=pltpu.SMEM)] * 2 + [pl.BlockSpec(memory_space=pl.ANY)] * group_size,
                out_specs=[pl.BlockSpec(memory_space=pl.ANY)] * group_size,
                scratch_shapes=[
                    pltpu.VMEM((count, LANES), jnp.float32),
                    pltpu.VMEM((count // fold, LANES), jnp.bfloat16),
                    pltpu.SMEM((count,), jnp.int32),
                    pltpu.SemaphoreType.DMA((group_size,)),
                    pltpu.SemaphoreType.DMA((group_size,)),
                    pltpu.SemaphoreType.DMA((group_size,)),
                ],
                compiler_params=pltpu.CompilerParams(vmem_limit_bytes=62 * 2**20),
                cost_estimate=estimate(c, 1_000_000_000),
            )(place, order, starts, spans, *rows)

        me = lax.axis_index('group')
        place = jnp.full((1,), me, jnp.int32)

        def shift(array, k):
            return lax.ppermute(array, 'group', [(i, (i + k) % group_size) for i in range(group_size)])

        halves = jnp.stack([sort_keys, (seg_ids >> 16).astype(jnp.float32), (seg_ids & 0xFFFF).astype(jnp.float32)])
        shifted = [halves] + [shift(halves, k) for k in range(1, group_size)]
        every = jnp.stack(shifted)
        owner = (me - jnp.arange(group_size, dtype=jnp.int32) + group_size) % group_size
        record = (owner[:, None] * rows_dev + jnp.arange(rows_dev, dtype=jnp.int32)[None, :]).reshape(count)
        keys = every[:, 0].reshape(count)
        ids = ((every[:, 1].astype(jnp.int32) << 16) | every[:, 2].astype(jnp.int32)).reshape(count)
        first = pack(0, payload)
        _, ids_sorted, order = lax.sort((keys, ids, record), num_keys=1, is_stable=False)
        new = jnp.concatenate([jnp.ones((1,), jnp.bool_), ids_sorted[1:] != ids_sorted[:-1]]).astype(jnp.int32)
        starts = jnp.sum(new.reshape(count // BITS, BITS) << jnp.arange(BITS, dtype=jnp.int32)[None, :], axis=1)
        spans = jnp.max(new.reshape(1, count // SPAN, SPAN), axis=2)
        order, starts, spans, folded = lax.optimization_barrier((order, starts, spans, payload))

        sent = [first] + [pack(c, folded) for c in range(1, len(FOLDS))]
        there = [[s[0]] + [shift(s[k], k) for k in range(1, group_size)] for s in sent]
        done = [walk(c, order, starts, spans, t) for c, t in enumerate(there)]
        back = [[d[0]] + [shift(d[k], group_size - k) for k in range(1, group_size)] for d in done]
        out = None
        for c, b in enumerate(back):
            out = unpack(c, b, out)
        return out

    row_spec = P(('batch', 'group'))
    mat_spec = P(('batch', 'group'), None)
    return jax.shard_map(per_device, mesh=mesh, in_specs=(row_spec, row_spec, mat_spec),
                         out_specs=mat_spec, check_vma=False)
```
